32 devices in a mesh: energy: 8 (over z, y), layer: 4 (over x, core).
Axes of the slice: x: 2, y: 2, z: 4, core: 2. Of those that a mesh axis runs over, the one named last changes fastest.
Arguments:
- layer_inverse: float32 [8, 32, 256, 256], P('energy', 'layer'), may hold values from -0.008125 to 1, as said below
- coupling: float32 [256, 256], replicated, may hold values from -0.5125 to 0.5125, as said below
- lead_left: float32 [8, 256, 256], P('energy'), may hold values from -0.0040625 to 0.5, as said below
- lead_right: float32 [8, 256, 256], P('energy'), may hold values from -0.0040625 to 0.5, as said below
- quad_weight: float32 [8], replicated, may hold values from 0.0125 to 0.5
- energy_slot: int32 [8], P('energy'), may hold values from 0 to 7, each once
- plane_of: int32 [32], replicated, may hold values from 0 to 127
- doping: float32 [128, 128, 128], P(('energy', 'layer')), may hold values from -6 to 6
- screening: float32 [128, 128, 128], P(('energy', 'layer')), may hold values from 0.25 to 2
Outputs:
- layer_density: float32 [32, 256], P('layer')
- potential: float32 [128, 128, 128], P(('energy', 'layer'))
- residual: float32 [128, 128, 128], P(('energy', 'layer'))
The draws below stay inside these ranges and needn't reach their ends.
Inputs may be any that keep to these rules, and one draw needn't show every extreme that they name: `layer_inverse`: each block is symmetric; its diagonal entries lie between 0.3 and 1.0 and its other entries within 0.13 * 256 ** -0.5 of zero. `coupling`: entries are independent with mean zero. `lead_left`: each block is symmetric; its diagonal entries lie between 0.15 and 0.5 and its other entries within 0.065 * 256 ** -0.5 of zero. `lead_right`: each block is symmetric; its diagonal entries lie between 0.15 and 0.5 and its other entries within 0.065 * 256 ** -0.5 of zero. `energy_slot`: every quadrature index appears once. `plane_of`: several layers may share a plane.
All inputs are finite; a program needn't handle non-finite values.
Results may differ from the reference program's by a relative error of at most 0.00018.
Values sent between devices are 32-bit elements; how exact they have to be, the bound alone decides.
A program may use at most 128 MiB of HBM per device.

```python
import math
from functools import partial
import jax
import jax.numpy as jnp
from jax import lax

M = 256
ORB_Y = 16
ORB_Z = 16
NY = 128
NZ = 128
LAYERS = 32
ENERGIES = 8
NX = 128
CG_ITERS = 3


def symmetric_blocks(key, lead_shape, factor):
    key_diag, key_off = jax.random.split(key)
    orbitals = M
    diag_values = jnp.exp(jax.random.uniform(key_diag, lead_shape + (orbitals,), jnp.float32, math.log(0.3), 0.0))
    half_width = 0.13 * orbitals ** (-0.5)
    noise = jax.random.uniform(key_off, lead_shape + (orbitals, orbitals), jnp.float32, -half_width, half_width)
    noise = 0.5 * (noise + jnp.swapaxes(noise, -1, -2))
    identity_mat = jnp.eye(orbitals, dtype=jnp.float32)
    blocks = noise * (1.0 - identity_mat) + diag_values[..., None] * identity_mat
    return (factor * blocks).astype(jnp.float32)


def draw_layer_inverse(key, part):
    return symmetric_blocks(jax.random.fold_in(key, 11), (ENERGIES, LAYERS), 1.0)


def draw_coupling(key, part):
    coupling_key = jax.random.fold_in(key, 14)
    spread = 1.36 * M ** (-0.5)
    values = jnp.clip(spread * jax.random.normal(coupling_key, (M, M), jnp.float32), -6.0 * spread, 6.0 * spread)
    return values.astype(jnp.float32)


def draw_lead_left(key, part):
    return symmetric_blocks(jax.random.fold_in(key, 12), (ENERGIES,), 0.5)


def draw_lead_right(key, part):
    return symmetric_blocks(jax.random.fold_in(key, 13), (ENERGIES,), 0.5)


def set_ends(drawn, rng, least, top_value):
    longest = drawn.shape.index(max(drawn.shape))
    spots = []
    for shift in (0, 1):
        where = [jax.random.randint(jax.random.fold_in(rng, axis), (), 0, length) for axis, length in enumerate(drawn.shape)]
        where[longest] = (where[longest] + shift) % drawn.shape[longest]
        spots.append(tuple(where))
    return drawn.at[spots[0]].set(least).at[spots[1]].set(top_value)


def shard_levels(key, shape, pieces, low, top_value):
    gain, own = 1.0, jax.random.fold_in(key, 6)
    for position, shards_of in pieces:
        steps = jnp.exp(jax.random.uniform(jax.random.fold_in(own, position), (shards_of,), jnp.float32, low / len(pieces), top_value / len(pieces)))
        gain = gain * jnp.repeat(steps, shape[position] // shards_of).reshape([-1 if axis == position else 1 for axis in range(len(shape))])
    return gain


def gaussian(key, shape, deviation, most, cuts=(), kind=jnp.bfloat16):
    array = jax.random.normal(key, shape, jnp.float32) * deviation
    if len(cuts) > 0:
        array = shard_levels(key, shape, cuts, -0.22, 0.18) * array
    return jnp.clip(array, min=-most, max=most).astype(kind)


def setup_inputs(seed: int = 0) -> dict:
    splits = jax.random.split(jax.random.key(seed), 10)
    return {
        "layer_inverse": draw_layer_inverse(jax.random.fold_in(splits[9], 71), 0),
        "coupling": draw_coupling(jax.random.fold_in(splits[9], 71), 0),
        "lead_left": draw_lead_left(jax.random.fold_in(splits[9], 71), 0),
        "lead_right": draw_lead_right(jax.random.fold_in(splits[9], 71), 0),
        "quad_weight": jnp.clip(jnp.exp(jax.random.uniform(splits[4], (ENERGIES,), jnp.float32, math.log(0.0125), math.log(0.5))), 0.0125, 0.5),
        "energy_slot": jax.random.permutation(splits[5], ENERGIES).astype(jnp.int32),
        "plane_of": set_ends(jax.random.randint(splits[6], (LAYERS,), 0, NX), jax.random.fold_in(splits[6], 1), 0, NX - 1).astype(jnp.int32),
        "doping": gaussian(splits[7], (NX, NY, NZ), 1.0, 6.0, ((0, 32),), jnp.float32),
        "screening": jnp.clip(0.25 + 1.75 * jax.random.uniform(splits[8], (NX, NY, NZ), jnp.float32) ** shard_levels(splits[8], (NX, NY, NZ), ((0, 32),), -0.2, 0.2), 0.25, 2.0),
    }


exact_mode = lax.Precision.HIGHEST


def matmul_hi(left_mat, right_mat):
    return jnp.matmul(left_mat, right_mat, precision=exact_mode)


def chain_diagonals(tmat, energy_item):
    inverse, left_lead, right_lead = energy_item
    forward = matmul_hi(inverse, tmat)
    backward = matmul_hi(inverse, tmat.T)

    def step_chain(state_mat, layer_pair):
        inv_layer, propagator = layer_pair
        following = inv_layer + matmul_hi(matmul_hi(propagator, state_mat), propagator.T)
        return following, state_mat

    _, left_in = lax.scan(step_chain, left_lead, (inverse, forward))
    _, right_in = lax.scan(step_chain, right_lead, (inverse, backward), reverse=True)
    self_energy = matmul_hi(matmul_hi(tmat, left_in), tmat.T) + matmul_hi(matmul_hi(tmat.T, right_in), tmat)
    dressed = matmul_hi(inverse, self_energy)
    return jnp.diagonal(inverse, axis1=1, axis2=2) + jnp.sum(dressed * jnp.swapaxes(inverse, 1, 2), axis=2)


def operate(values_in, screening):
    padded = jnp.pad(values_in, 1)
    beside = padded[2:, 1:-1, 1:-1] + padded[:-2, 1:-1, 1:-1]
    beside = beside + padded[1:-1, 2:, 1:-1] + padded[1:-1, :-2, 1:-1]
    beside = beside + padded[1:-1, 1:-1, 2:] + padded[1:-1, 1:-1, :-2]
    return (6.0 + screening) * values_in - beside


def reference(layer_inverse, coupling, lead_left, lead_right, quad_weight, energy_slot, plane_of, doping, screening):
    diagonals = lax.map(partial(chain_diagonals, coupling), (layer_inverse, lead_left, lead_right))
    weight = quad_weight[energy_slot]
    layer_density = jnp.sum(weight[:, None, None] * diagonals, axis=0)
    plane_ids = jnp.arange(NX, dtype=jnp.int32)
    onehot = (plane_of[None, :] == plane_ids[:, None]).astype(jnp.float32)
    plane_charge = jnp.dot(onehot, layer_density, precision=exact_mode).reshape(NX, ORB_Y, ORB_Z)
    charge = jnp.repeat(jnp.repeat(plane_charge, NY // ORB_Y, axis=1), NZ // ORB_Z, axis=2)
    source = charge - doping
    potential = jnp.zeros_like(source)
    residual, direction = source, source
    norm_now = jnp.sum(residual * residual)
    for iteration in range(CG_ITERS):
        applied = operate(direction, screening)
        step_size = norm_now / jnp.sum(direction * applied)
        potential = potential + step_size * direction
        residual = residual - step_size * applied
        norm_next = jnp.sum(residual * residual)
        direction = residual + (norm_next / norm_now) * direction
        norm_now = norm_next
    return layer_density, potential, residual
```

```python
import functools
import jax
import jax.numpy as jnp
from jax import lax
from jax.experimental import pallas as pl
from jax.experimental.pallas import tpu as pltpu
from jax.sharding import PartitionSpec as P

ORB_Y = 16
CG_ITERS = 3
CENTER = 7.125
HALF = 7.0
F32 = jnp.float32
BF16 = jnp.bfloat16
LOGICAL = pl.DeviceIdType.LOGICAL


def split(x):
    hi = x.astype(BF16)
    lo = (x - hi.astype(F32)).astype(BF16)
    return hi, lo


def mm(a, b):
    return jnp.dot(a, b, preferred_element_type=F32)


def mm3(a, b):
    return mm(a[0], b[0]) + mm(a[0], b[1]) + mm(a[1], b[0])


def loop(count, step):
    if count <= 32:
        for k in range(1, count):
            step(k, 0)
    else:
        lax.fori_loop(1, count, step, 0)


def beside_of(v, prev_z, next_z):
    inner = v[1:-1]
    n, ny, nz = inner.shape
    total = v[2:] + v[:-2]
    yi = lax.broadcasted_iota(jnp.int32, (1, ny, 1), 1)
    zi = lax.broadcasted_iota(jnp.int32, (1, 1, nz), 2)
    total += jnp.where(yi == 0, 0.0, pltpu.roll(inner, 1, 1))
    total += jnp.where(yi == ny - 1, 0.0, pltpu.roll(inner, ny - 1, 1))
    total += jnp.where(zi == 0, 0.0, pltpu.roll(inner, 1, 2))
    total += jnp.where(zi == nz - 1, 0.0, pltpu.roll(inner, nz - 1, 2))
    return total


def kernel(
    n_energy, n_layer,
    d_hbm, t_hbm, lead_l_hbm, lead_r_hbm, qw_hbm, slot_ref, plane_hbm, dop_hbm, scr_hbm,
    dens_ref, pot_ref, res_ref,
    d_ref, t_ref, qw_ref, plane_ref, dop_ref, scr_ref, in_sem,
    prop_ref, ct_ref, c_ref, s_ref, diag_ref, full_ref, gin, gout, dop_ext, scr_ext,
    redbuf, rows_buf, mom,
    relay_send, relay_recv, halo_send, halo_recv,
    red_send, red_recv, row_send, row_recv, mom_send, mom_recv,
):
    steps, m, _ = d_hbm.shape
    planes, ny, nz = dop_hbm.shape
    halo = CG_ITERS
    ext = planes + 2 * halo
    total = n_energy * n_layer
    e = lax.axis_index("energy")
    i = lax.axis_index("layer")
    lin = e * n_layer + i
    up = lax.rem(lin + 1, total)
    down = lax.rem(lin + total - 1, total)

    order = []
    for s in range((steps + 1) // 2):
        order += [s] if s == steps - 1 - s else [s, steps - 1 - s]
    t_copy = pltpu.make_async_copy(t_hbm, t_ref, in_sem.at[steps + 4])
    t_copy.start()
    for s in order:
        pltpu.make_async_copy(d_hbm.at[s], d_ref.at[s], in_sem.at[s]).start()
    grid_copies = [
        pltpu.make_async_copy(qw_hbm, qw_ref, in_sem.at[steps + 5]),
        pltpu.make_async_copy(plane_hbm, plane_ref, in_sem.at[steps + 6]),
        pltpu.make_async_copy(dop_hbm, dop_ref, in_sem.at[steps]),
        pltpu.make_async_copy(scr_hbm, scr_ref, in_sem.at[steps + 1]),
    ]
    for copy in grid_copies:
        copy.start()

    @pl.when(i == 0)
    def _():
        pltpu.make_async_copy(lead_l_hbm, gin.at[0], in_sem.at[steps + 2]).start()

    @pl.when(i == n_layer - 1)
    def _():
        pltpu.make_async_copy(lead_r_hbm, gin.at[1], in_sem.at[steps + 3]).start()

    barrier = pltpu.get_barrier_semaphore()

    def greet(k, c):
        pl.semaphore_signal(barrier, inc=1, device_id=lax.rem(lin + k, total), device_id_type=LOGICAL)
        return c

    loop(total, greet)

    halo_copies = []
    for j, (src, dst, width) in enumerate(((dop_ref, dop_ext, halo), (scr_ref, scr_ext, halo - 1))):
        halo_copies.append(pltpu.make_async_remote_copy(
            src_ref=src.at[pl.ds(planes - width, width)], dst_ref=dst.at[pl.ds(halo - width, width)],
            send_sem=halo_send.at[2 * j], recv_sem=halo_recv.at[2 * j],
            device_id=up, device_id_type=LOGICAL))
        halo_copies.append(pltpu.make_async_remote_copy(
            src_ref=src.at[pl.ds(0, width)], dst_ref=dst.at[pl.ds(planes + halo, width)],
            send_sem=halo_send.at[2 * j + 1], recv_sem=halo_recv.at[2 * j + 1],
            device_id=down, device_id_type=LOGICAL))

    t_copy.wait()
    t = t_ref[...]
    tt = t.T
    t, tt = split(t), split(tt)
    eye = (lax.broadcasted_iota(jnp.int32, (m // 2, m // 2), 0)
           == lax.broadcasted_iota(jnp.int32, (m // 2, m // 2), 1))

    def diag_row(x):
        h = m // 2
        tiles = [jnp.where(eye, x[k * h : k * h + h, k * h : k * h + h], 0.0) for k in range(2)]
        return jnp.concatenate([jnp.sum(tile, axis=0, keepdims=True) for tile in tiles], axis=1)

    sides = ((t, tt), (tt, t))

    def layer_of(side, s):
        return s if side == 0 else steps - 1 - s

    def layer_copy(s):
        return pltpu.make_async_copy(d_hbm.at[s], d_ref.at[s], in_sem.at[s])

    def prepare(s, side):
        d_s = split(d_ref[layer_of(side, s)])
        right, left = sides[side]
        prop = mm3(d_s, right)
        for j, half in enumerate(split(prop)):
            prop_ref[side, j] = half
        for j, half in enumerate(split(prop.T)):
            prop_ref[side, 2 + j] = half

    def advance(s, side, ahead):
        prop = (prop_ref[side, 0], prop_ref[side, 1])
        prop_t = (prop_ref[side, 2], prop_ref[side, 3])
        half = mm3(split(s_ref[side]), prop_t)
        carry = mm3(split(ct_ref[side, s - 1]), prop_t)
        acc = d_ref[layer_of(side, s)] + mm3(prop, split(half))
        ct_ref[side, s] = carry
        s_ref[side] = acc
        diag_ref[side, pl.ds(s, 1), :] = diag_row(acc)
        if side == 0:
            full_ref[pl.ds(s, 1), :] = diag_row(d_ref[s])
        if ahead:
            prepare(s + 1, side)

    def step(s, c):
        for side in range(2):
            advance(s, side, True)
        return c

    def step_wait(s, c):
        layer_copy(s + 1).wait()
        layer_copy(steps - 2 - s).wait()
        return step(s, c)

    for s in (0, 1):
        layer_copy(s).wait()
        layer_copy(steps - 1 - s).wait()
    for side in range(2):
        d = d_ref[layer_of(side, 0)]
        s_ref[side] = d
        ct_ref[side, 0] = mm3(sides[side][1], split(d))
        diag_ref[side, 0:1, :] = diag_row(d)
        if side == 0:
            full_ref[0:1, :] = diag_row(d)
        prepare(1, side)
    lax.fori_loop(1, steps // 2 - 1, step_wait, 0)
    pl.semaphore_wait(barrier, total - 1)
    for copy in grid_copies:
        copy.wait()
    for copy in halo_copies:
        copy.start()
    lax.fori_loop(steps // 2 - 1, steps - 1, step, 0)
    for side in range(2):
        advance(steps - 1, side, False)
        c_ref[side] = ct_ref[side, steps - 1].T

    @pl.when(i == 0)
    def _():
        pltpu.make_async_copy(lead_l_hbm, gin.at[0], in_sem.at[steps + 2]).wait()

    @pl.when(i == n_layer - 1)
    def _():
        pltpu.make_async_copy(lead_r_hbm, gin.at[1], in_sem.at[steps + 3]).wait()

    h = m // 2

    def relay_copy(side, part):
        spot = (pl.ds(0, h), pl.ds(0, m)) if part == 0 else (pl.ds(h, h), pl.ds(h, h))
        return pltpu.make_async_remote_copy(
            src_ref=gout.at[(side,) + spot], dst_ref=gin.at[(side,) + spot],
            send_sem=relay_send.at[side, part], recv_sem=relay_recv.at[side, part],
            device_id=e * n_layer + lax.rem(i + 1 - 2 * side + n_layer, n_layer), device_id_type=LOGICAL)

    first = (2 * i) // n_layer
    def turn_step(turn, c):
        side = first + turn * (1 - 2 * first)
        pos = i + side * (n_layer - 1 - 2 * i)

        @pl.when(pos > 0)
        def _():
            relay_copy(side, 0).wait_recv()
            gin[side, h:, :h] = gin[side, :h, h:].T
            relay_copy(side, 1).wait_recv()

        @pl.when(pos < n_layer - 1)
        def _():
            half = split(mm3(split(gin[side]), split(ct_ref[side, steps - 1])))
            outer = split(c_ref[side])
            gout[side, :h, :] = s_ref[side, :h, :] + mm3([x[:h] for x in outer], half)
            relay_copy(side, 0).start()
            gout[side, h:, h:] = s_ref[side, h:, h:] + mm3([x[h:] for x in outer], [x[:, h:] for x in half])
            relay_copy(side, 1).start()

        g = split(gin[side])
        for s in range(steps):
            carry = ct_ref[side, s]
            z = mm3(g, split(carry))
            diag_ref[side, s : s + 1, :] += jnp.sum(z * carry, axis=0, keepdims=True)
        return c

    lax.fori_loop(0, 2, turn_step, 0)

    n_slots = qw_ref.shape[1]
    pick = lax.broadcasted_iota(jnp.int32, (1, n_slots), 1) == slot_ref[...]
    weight = jnp.sum(jnp.where(pick, qw_ref[...], 0.0), axis=1, keepdims=True)
    back = jnp.concatenate([diag_ref[1, steps - 1 - s : steps - s, :] for s in range(steps)], axis=0)
    redbuf[e] = weight * (diag_ref[0] + back - full_ref[...])

    def exchange(buf, me, count, place, send_sem, recv_sem):
        def send(k, c):
            pltpu.make_async_remote_copy(
                src_ref=buf.at[me], dst_ref=buf.at[me], send_sem=send_sem, recv_sem=recv_sem,
                device_id=place(lax.rem(me + k, count)), device_id_type=LOGICAL).start()
            return c

        loop(count, send)
        rest = buf.at[pl.ds(0, count - 1)]
        return pltpu.make_async_remote_copy(
            src_ref=rest, dst_ref=rest, send_sem=send_sem, recv_sem=recv_sem,
            device_id=place(lax.rem(me + 1, count)), device_id_type=LOGICAL)

    def ordered_sum(ref, count):
        if count <= 8:
            out = ref[0]
            for k in range(1, count):
                out = out + ref[k]
            return out
        return lax.fori_loop(1, count, lambda k, c: c + ref[k], ref[0])

    red = exchange(redbuf, e, n_energy, lambda p: p * n_layer + i, red_send, red_recv)
    red.wait_recv()
    own = ordered_sum(redbuf, n_energy)
    dens_ref[...] = own
    rows_buf[i] = own
    row = exchange(rows_buf, i, n_layer, lambda p: e * n_layer + p, row_send, row_recv)
    red.wait_send()
    row.wait_recv()
    row.wait_send()

    dop_ext[halo : halo + planes] = dop_ref[...]
    scr_ext[halo : halo + planes] = scr_ref[...]
    for copy in halo_copies:
        copy.wait_recv()
    rows = rows_buf[...].reshape(n_layer * steps, m)
    orb_z = m // ORB_Y
    padded = -(-ext // 8) * 8
    first_plane = lin * planes - halo
    ids = first_plane + lax.broadcasted_iota(jnp.int32, (padded, 1), 0)
    onehot = (plane_ref[...] == ids).astype(F32)
    charge_rows = jnp.dot(onehot, rows, precision=lax.Precision.HIGHEST, preferred_element_type=F32)
    ysel = (lax.broadcasted_iota(jnp.int32, (ny, m), 1) // orb_z
            == lax.broadcasted_iota(jnp.int32, (ny, m), 0) // (ny // ORB_Y))
    zsel = (lax.broadcasted_iota(jnp.int32, (m, nz), 1) // (nz // orb_z)
            == lax.rem(lax.broadcasted_iota(jnp.int32, (m, nz), 0), orb_z)).astype(BF16)
    spreads = jnp.concatenate(
        [jnp.where(ysel, charge_rows[p : p + 1, :], 0.0) for p in range(ext)], axis=0)
    hi, lo = split(spreads)
    charge = (mm(hi, zsel) + mm(lo, zsel)).reshape(ext, ny, nz)
    last_plane = total * planes
    gid = first_plane + lax.broadcasted_iota(jnp.int32, (ext, 1, 1), 0)
    inside = jnp.logical_and(gid >= 0, gid < last_plane)
    v0 = jnp.where(inside, charge - dop_ext[...], 0.0)

    basis = [v0]
    for k in range(CG_ITERS):
        prev = basis[-1]
        scr = scr_ext[k + 1 : ext - k - 1]
        shifted = ((6.0 - CENTER + scr) * prev[1:-1] - beside_of(prev, None, None)) * (1.0 / HALF)
        if k > 0:
            shifted = 2.0 * shifted - basis[-2][2:-2]
        mask = inside[k + 1 : ext - k - 1]
        basis.append(jnp.where(mask, shifted, 0.0))
    own_v = [b[halo - k : halo - k + planes] for k, b in enumerate(basis)]
    names, parts = {}, []
    for a in range(CG_ITERS):
        for b in range(a, CG_ITERS + 1):
            names[a, b] = len(parts)
            parts.append(jnp.sum(own_v[a] * own_v[b], axis=(0, 1), keepdims=True)[0])
    parts.append(jnp.zeros((16 - len(parts), nz), F32))
    column = jnp.sum(jnp.concatenate(parts, axis=0), axis=1, keepdims=True)
    spot = lax.broadcasted_iota(jnp.int32, (16, nz), 0) == lax.broadcasted_iota(jnp.int32, (16, nz), 1)
    mom[lin] = jnp.sum(jnp.where(spot, column, 0.0), axis=0, keepdims=True)

    sums = exchange(mom, lin, total, lambda p: p, mom_send, mom_recv)
    for copy in halo_copies:
        copy.wait_send()
    sums.wait_send()
    for side in range(2):
        pos = i + side * (n_layer - 1 - 2 * i)

        @pl.when(pos < n_layer - 1)
        def _():
            relay_copy(side, 0).wait_send()
            relay_copy(side, 1).wait_send()

    sums.wait_recv()
    gram = jnp.sum(mom[...].reshape(total, nz), axis=0, keepdims=True)

    def entry(a, b):
        k = names[min(a, b), max(a, b)]
        return gram[:, k : k + 1]

    def inner(x, y):
        terms = [x[a] * y[b] * entry(a, b) for a in x for b in y]
        return functools.reduce(lambda p, q: p + q, terms)

    def add(x, y, scale):
        out = dict(x)
        for k, val in y.items():
            out[k] = out[k] + scale * val if k in out else scale * val
        return out

    def apply(x):
        out = {}
        for k, val in x.items():
            out = add(out, {k: val}, CENTER)
            if k == 0:
                out = add(out, {1: val}, HALF)
            else:
                out = add(out, {k + 1: val, k - 1: val}, 0.5 * HALF)
        return out

    one = jnp.ones((1, 1), F32)
    pot, res, direction = {}, {0: one}, {0: one}
    norm = inner(res, res)
    for it in range(CG_ITERS):
        applied = apply(direction)
        step = norm / inner(direction, applied)
        pot = add(pot, direction, step)
        res = add(res, applied, -step)
        if it + 1 < CG_ITERS:
            new = inner(res, res)
            direction = add(res, direction, new / norm)
            norm = new

    for coefs, out in ((pot, pot_ref), (res, res_ref)):
        terms = [coefs[k][None] * own_v[k] for k in coefs]
        out[...] = functools.reduce(lambda p, q: p + q, terms)


def put(dens_ref, pot_ref, res_ref, dens_hbm, pot_hbm, res_hbm, sem):
    copies = [
        pltpu.make_async_copy(src, dst, sem.at[k])
        for k, (src, dst) in enumerate(((pot_ref, pot_hbm), (res_ref, res_hbm), (dens_ref, dens_hbm)))
    ]
    for copy in copies:
        copy.start()
    for copy in copies:
        copy.wait()


def body(n_energy, n_layer, layer_inverse, coupling, lead_left, lead_right, quad_weight,
         energy_slot, plane_of, doping, screening):
    steps, m = layer_inverse.shape[1], layer_inverse.shape[2]
    planes, ny, nz = doping.shape
    ext = planes + 2 * CG_ITERS
    dma = pltpu.SemaphoreType.DMA
    vmem = pl.BlockSpec(memory_space=pltpu.VMEM)
    anym = pl.BlockSpec(memory_space=pltpu.HBM)
    call = pl.pallas_call(
        functools.partial(kernel, n_energy, n_layer),
        out_shape=(pltpu.VMEM((steps, m), F32), pltpu.VMEM(doping.shape, F32), pltpu.VMEM(doping.shape, F32)),
        in_specs=[anym] * 5 + [vmem] + [anym] * 3,
        out_specs=(vmem, vmem, vmem),
        scratch_shapes=[
            pltpu.VMEM((steps, m, m), F32),
            pltpu.VMEM((m, m), F32),
            pltpu.VMEM((1,) + quad_weight.shape, F32),
            pltpu.VMEM((1,) + plane_of.shape, jnp.int32),
            pltpu.VMEM(doping.shape, F32),
            pltpu.VMEM(doping.shape, F32),
            dma((steps + 7,)),
            pltpu.VMEM((2, 4, m, m), BF16),
            pltpu.VMEM((2, steps, m, m), F32),
            pltpu.VMEM((2, m, m), F32),
            pltpu.VMEM((2, m, m), F32),
            pltpu.VMEM((2, steps, m), F32),
            pltpu.VMEM((steps, m), F32),
            pltpu.VMEM((2, m, m), F32),
            pltpu.VMEM((2, m, m), F32),
            pltpu.VMEM((ext, ny, nz), F32),
            pltpu.VMEM((ext, ny, nz), F32),
            pltpu.VMEM((n_energy, steps, m), F32),
            pltpu.VMEM((n_layer, steps, m), F32),
            pltpu.VMEM((n_energy * n_layer, 1, nz), F32),
            dma((2, 2)), dma((2, 2)), dma((4,)), dma((4,)),
            dma, dma, dma, dma, dma, dma,
        ],
        compiler_params=pltpu.CompilerParams(
            collective_id=0, has_side_effects=True, vmem_limit_bytes=66_000_000
        ),
    )
    inner = call(
        layer_inverse[0], coupling, lead_left[0], lead_right[0], quad_weight[None, :],
        energy_slot[:, None], plane_of[None, :], doping, screening,
    )
    return pl.pallas_call(
        put,
        out_shape=tuple(jax.ShapeDtypeStruct(x.shape, F32) for x in inner),
        in_specs=[vmem] * 3,
        out_specs=(anym, anym, anym),
        scratch_shapes=[dma((3,))],
        compiler_params=pltpu.CompilerParams(vmem_limit_bytes=1_000_000),
    )(*(pltpu.with_memory_space_constraint(x, pltpu.VMEM) for x in inner))


def solution(mesh):
    in_specs = (
        P("energy", "layer", None, None),
        P(),
        P("energy", None, None),
        P("energy", None, None),
        P(),
        P("energy"),
        P(),
        P(("energy", "layer"), None, None),
        P(("energy", "layer"), None, None),
    )
    out_specs = (
        P("layer", None),
        P(("energy", "layer"), None, None),
        P(("energy", "layer"), None, None),
    )
    run = functools.partial(body, mesh.shape["energy"], mesh.shape["layer"])
    return jax.shard_map(run, mesh=mesh, in_specs=in_specs, out_specs=out_specs, check_vma=False)
```

```python
import functools
import jax
import jax.numpy as jnp
from jax import lax
from jax.experimental import pallas as pl
from jax.experimental.pallas import tpu as pltpu
from jax.sharding import PartitionSpec as P

ORB_Y = 16
CG_ITERS = 3
CENTER = 7.125
HALF = 7.0
F32 = jnp.float32
BF16 = jnp.bfloat16
LOGICAL = pl.DeviceIdType.LOGICAL


def split(x):
    hi = x.astype(BF16)
    lo = (x - hi.astype(F32)).astype(BF16)
    return hi, lo


def mm(a, b):
    return jnp.dot(a, b, preferred_element_type=F32)


def mm3(a, b, dot=mm):
    return dot(a[0], b[0]) + dot(a[0], b[1]) + dot(a[1], b[0])


def mmt(a, b):
    return lax.dot_general(a, b, (((1,), (1,)), ((), ())), preferred_element_type=F32)


def loop(count, step):
    if count <= 32:
        for k in range(1, count):
            step(k, 0)
    else:
        lax.fori_loop(1, count, step, 0)


def beside_of(v, prev_z, next_z):
    inner = v[1:-1]
    n, ny, nz = inner.shape
    total = v[2:] + v[:-2]
    yi = lax.broadcasted_iota(jnp.int32, (1, ny, 1), 1)
    zi = lax.broadcasted_iota(jnp.int32, (1, 1, nz), 2)
    total += jnp.where(yi == 0, 0.0, pltpu.roll(inner, 1, 1))
    total += jnp.where(yi == ny - 1, 0.0, pltpu.roll(inner, ny - 1, 1))
    total += jnp.where(zi == 0, 0.0, pltpu.roll(inner, 1, 2))
    total += jnp.where(zi == nz - 1, 0.0, pltpu.roll(inner, nz - 1, 2))
    return total


def kernel(
    n_energy, n_layer,
    d_hbm, t_hbm, lead_l_hbm, lead_r_hbm, qw_hbm, slot_hbm, plane_hbm, dop_hbm, scr_hbm,
    dens_ref, pot_ref, res_ref,
    d_ref, t_ref, qw_ref, slot_ref, plane_ref, dop_ref, scr_ref, in_sem,
    p_ref, s_ref, ct_ref, c_ref, w_ref, x_ref, diag_ref, full_ref, gin, gout, dop_ext, scr_ext,
    zbuf, redbuf, mom,
    relay_send, relay_recv, halo_send, halo_recv,
    z_send, z_recv, red_send, red_recv, mom_send, mom_recv,
):
    steps, m, _ = d_hbm.shape
    planes, ny, nz = dop_hbm.shape
    halo = CG_ITERS
    ext = planes + 2 * halo
    total = n_energy * n_layer
    e = lax.axis_index("energy")
    i = lax.axis_index("layer")
    lin = e * n_layer + i
    up = lax.rem(lin + 1, total)
    down = lax.rem(lin + total - 1, total)

    order = []
    for s in range((steps + 1) // 2):
        order += [s] if s == steps - 1 - s else [s, steps - 1 - s]
    t_copy = pltpu.make_async_copy(t_hbm, t_ref, in_sem.at[steps + 4])
    t_copy.start()

    def layer_copy(s):
        return pltpu.make_async_copy(d_hbm.at[s], d_ref.at[s], in_sem.at[s])

    def lead_copy(side):
        return pltpu.make_async_copy((lead_l_hbm, lead_r_hbm)[side], s_ref.at[side], in_sem.at[steps + 2 + side])

    ends = (0, n_layer - 1)
    for s in order[:2]:
        layer_copy(s).start()
    for side in range(2):
        pl.when(i == ends[side])(lead_copy(side).start)
    for s in order[2:]:
        layer_copy(s).start()
    grid_copies = [
        pltpu.make_async_copy(qw_hbm, qw_ref, in_sem.at[steps + 5]),
        pltpu.make_async_copy(plane_hbm, plane_ref, in_sem.at[steps + 6]),
        pltpu.make_async_copy(slot_hbm, slot_ref, in_sem.at[steps + 7]),
        pltpu.make_async_copy(dop_hbm, dop_ref, in_sem.at[steps]),
        pltpu.make_async_copy(scr_hbm, scr_ref, in_sem.at[steps + 1]),
    ]
    for copy in grid_copies:
        copy.start()

    barrier = pltpu.get_barrier_semaphore()

    def greet(k, c):
        pl.semaphore_signal(barrier, inc=1, device_id=lax.rem(lin + k, total), device_id_type=LOGICAL)
        return c

    loop(total, greet)

    halo_copies = []
    for j, (src, dst, width) in enumerate(((dop_ref, dop_ext, halo), (scr_ref, scr_ext, halo - 1))):
        halo_copies.append(pltpu.make_async_remote_copy(
            src_ref=src.at[pl.ds(planes - width, width)], dst_ref=dst.at[pl.ds(halo - width, width)],
            send_sem=halo_send.at[2 * j], recv_sem=halo_recv.at[2 * j],
            device_id=up, device_id_type=LOGICAL))
        halo_copies.append(pltpu.make_async_remote_copy(
            src_ref=src.at[pl.ds(0, width)], dst_ref=dst.at[pl.ds(planes + halo, width)],
            send_sem=halo_send.at[2 * j + 1], recv_sem=halo_recv.at[2 * j + 1],
            device_id=down, device_id_type=LOGICAL))

    t_copy.wait()
    t = t_ref[...]
    tt = t.T
    t, tt = split(t), split(tt)
    eye = (lax.broadcasted_iota(jnp.int32, (m // 2, m // 2), 0)
           == lax.broadcasted_iota(jnp.int32, (m // 2, m // 2), 1))

    def diag_row(x):
        h = m // 2
        tiles = [jnp.where(eye, x[k * h : k * h + h, k * h : k * h + h], 0.0) for k in range(2)]
        return jnp.concatenate([jnp.sum(tile, axis=0, keepdims=True) for tile in tiles], axis=1)

    sides = ((t, tt), (tt, t))
    h = m // 2
    last = steps - 1

    def layer_of(side, s):
        return s if side == 0 else last - s

    def pair(ref, at):
        return ref[at + (0,)], ref[at + (1,)]

    def prepare(s, side):
        prop = mm3(split(d_ref[layer_of(side, s)]), sides[side][0])
        for j, x in enumerate(split(prop)):
            p_ref[side, s % 2, j] = x

    def store_carry(s, side, ct):
        hi, lo = split(ct)
        ct_ref[side, s, 0] = hi
        ct_ref[side, s, 1] = lo
        w_ref[side, s] = 2.0 * ct - hi.astype(F32)

    for side in range(2):
        @pl.when(i != ends[side])
        def _():
            s_ref[side] = jnp.zeros((m, m), F32)
    for s in order[:2]:
        layer_copy(s).wait()
    for side in range(2):
        prepare(0, side)
    for s in order[2:]:
        layer_copy(s).wait()
    for side in range(2):
        pl.when(i == ends[side])(lead_copy(side).wait)

    for s in range(steps):
        props = [pair(p_ref, (side, s % 2)) for side in range(2)]
        halves = [mm3(props[side], split(s_ref[side])) for side in range(2)]
        if s < last:
            for side in range(2):
                prepare(s + 1, side)
        for side in range(2):
            d = d_ref[layer_of(side, s)]
            acc = d + mm3(split(halves[side]), props[side], mmt)
            s_ref[side] = acc
            diag_ref[side, s : s + 1, :] = diag_row(acc)
            if side == 0:
                full_ref[s : s + 1, :] = diag_row(d)
        for side in range(2):
            if s == 0:
                hi, lo = (x.T for x in props[side])
                ct_ref[side, 0, 0] = hi
                ct_ref[side, 0, 1] = lo
                w_ref[side, 0] = hi.astype(F32) + 2.0 * lo.astype(F32)
            else:
                store_carry(s, side, mm3(pair(ct_ref, (side, s - 1)), props[side], mmt))
        if s == 1:
            pl.semaphore_wait(barrier, total - 1)
            for copy in grid_copies:
                copy.wait()
            for copy in halo_copies:
                copy.start()

    def relay_copy(side, part, buf):
        spot = (pl.ds(0, h), pl.ds(0, m)) if part == 0 else (pl.ds(h, h), pl.ds(h, h))
        return pltpu.make_async_remote_copy(
            src_ref=buf.at[spot], dst_ref=gin.at[(side,) + spot],
            send_sem=relay_send.at[side, part], recv_sem=relay_recv.at[side, part],
            device_id=e * n_layer + lax.rem(i + 1 - 2 * side + n_layer, n_layer), device_id_type=LOGICAL)

    for side in range(2):
        @pl.when(i == ends[side])
        def _():
            for part in range(2):
                relay_copy(side, part, s_ref.at[side]).start()

    for side in range(2):
        for part in range(2):
            c_ref[side, part] = ct_ref[side, last, part].T

    first = (2 * i) // n_layer

    def turn_step(turn, c):
        side = first + turn * (1 - 2 * first)
        pos = i + side * (n_layer - 1 - 2 * i)

        @pl.when(pos > 0)
        def _():
            relay_copy(side, 0, gout.at[side]).wait_recv()
            gin[side, h:, :h] = gin[side, :h, h:].T
            relay_copy(side, 1, gout.at[side]).wait_recv()
            for part, x in enumerate(split(gin[side])):
                x_ref[part] = x

            @pl.when(pos < n_layer - 1)
            def _():
                half = split(mm3((x_ref[0], x_ref[1]), pair(ct_ref, (side, last))))
                outer = pair(c_ref, (side,))
                gout[side, :h, :] = s_ref[side, :h, :] + mm3([x[:h] for x in outer], half)
                relay_copy(side, 0, gout.at[side]).start()
                gout[side, h:, h:] = (
                    s_ref[side, h:, h:] + mm3([x[h:] for x in outer], [x[:, h:] for x in half]))
                relay_copy(side, 1, gout.at[side]).start()

            for s in range(steps):
                carry = ct_ref[side, s, 0]
                z = mm(x_ref[0], carry) + mm(x_ref[1], carry)
                diag_ref[side, s : s + 1, :] += jnp.sum(z * w_ref[side, s], axis=0, keepdims=True)

        return c

    lax.fori_loop(0, 2, turn_step, 0)

    n_slots = qw_ref.shape[1]
    pick = lax.broadcasted_iota(jnp.int32, (1, n_slots), 1) == slot_ref[...]
    weight = jnp.sum(jnp.where(pick, qw_ref[...], 0.0), axis=1, keepdims=True)
    back = jnp.concatenate([diag_ref[1, steps - 1 - s : steps - s, :] for s in range(steps)], axis=0)
    near = 2 if n_energy % 2 == 0 else 1
    far = n_energy // near
    zed = e // near
    ring = near * n_layer
    own = lax.rem(lin, ring)
    zbuf[zed] = weight * (diag_ref[0] + back - full_ref[...])

    def exchange(buf, me, count, place, send_sem, recv_sem):
        def send(k, c):
            pltpu.make_async_remote_copy(
                src_ref=buf.at[me], dst_ref=buf.at[me], send_sem=send_sem, recv_sem=recv_sem,
                device_id=place(lax.rem(me + k, count)), device_id_type=LOGICAL).start()
            return c

        loop(count, send)
        rest = buf.at[pl.ds(0, count - 1)]
        return pltpu.make_async_remote_copy(
            src_ref=rest, dst_ref=rest, send_sem=send_sem, recv_sem=recv_sem,
            device_id=place(lax.rem(me + 1, count)), device_id_type=LOGICAL)

    def ordered_sum(ref, count, start=0, stride=1):
        if count <= 8:
            out = ref[start]
            for k in range(1, count):
                out = out + ref[start + k * stride]
            return out
        return lax.fori_loop(1, count, lambda k, c: c + ref[start + k * stride], ref[start])

    wide = exchange(zbuf, zed, far, lambda p: p * ring + own, z_send, z_recv)
    wide.wait_recv()
    redbuf[own] = ordered_sum(zbuf, far)
    red = exchange(redbuf, own, ring, lambda p: zed * ring + p, red_send, red_recv)
    wide.wait_send()
    red.wait_recv()
    red.wait_send()
    rows = [ordered_sum(redbuf, near, k, n_layer) for k in range(n_layer)]
    dens_ref[...] = ordered_sum(redbuf, near, i, n_layer)

    dop_ext[halo : halo + planes] = dop_ref[...]
    scr_ext[halo : halo + planes] = scr_ref[...]
    for copy in halo_copies:
        copy.wait_recv()
    rows = jnp.concatenate(rows, axis=0)
    orb_z = m // ORB_Y
    padded = -(-ext // 8) * 8
    first_plane = lin * planes - halo
    ids = first_plane + lax.broadcasted_iota(jnp.int32, (padded, 1), 0)
    onehot = (plane_ref[...] == ids).astype(F32)
    charge_rows = jnp.dot(onehot, rows, precision=lax.Precision.HIGHEST, preferred_element_type=F32)
    ysel = (lax.broadcasted_iota(jnp.int32, (ny, m), 1) // orb_z
            == lax.broadcasted_iota(jnp.int32, (ny, m), 0) // (ny // ORB_Y))
    zsel = (lax.broadcasted_iota(jnp.int32, (m, nz), 1) // (nz // orb_z)
            == lax.rem(lax.broadcasted_iota(jnp.int32, (m, nz), 0), orb_z)).astype(BF16)
    spreads = jnp.concatenate(
        [jnp.where(ysel, charge_rows[p : p + 1, :], 0.0) for p in range(ext)], axis=0)
    hi, lo = split(spreads)
    charge = (mm(hi, zsel) + mm(lo, zsel)).reshape(ext, ny, nz)
    last_plane = total * planes
    gid = first_plane + lax.broadcasted_iota(jnp.int32, (ext, 1, 1), 0)
    inside = jnp.logical_and(gid >= 0, gid < last_plane)
    v0 = jnp.where(inside, charge - dop_ext[...], 0.0)

    basis = [v0]
    for k in range(CG_ITERS):
        prev = basis[-1]
        scr = scr_ext[k + 1 : ext - k - 1]
        shifted = ((6.0 - CENTER + scr) * prev[1:-1] - beside_of(prev, None, None)) * (1.0 / HALF)
        if k > 0:
            shifted = 2.0 * shifted - basis[-2][2:-2]
        mask = inside[k + 1 : ext - k - 1]
        basis.append(jnp.where(mask, shifted, 0.0))
    own_v = [b[halo - k : halo - k + planes] for k, b in enumerate(basis)]
    names, parts = {}, []
    for a in range(CG_ITERS):
        for b in range(a, CG_ITERS + 1):
            names[a, b] = len(parts)
            parts.append(jnp.sum(own_v[a] * own_v[b], axis=(0, 1), keepdims=True)[0])
    parts.append(jnp.zeros((16 - len(parts), nz), F32))
    column = jnp.sum(jnp.concatenate(parts, axis=0), axis=1, keepdims=True)
    spot = lax.broadcasted_iota(jnp.int32, (16, nz), 0) == lax.broadcasted_iota(jnp.int32, (16, nz), 1)
    mom[lin] = jnp.sum(jnp.where(spot, column, 0.0), axis=0, keepdims=True)

    sums = exchange(mom, lin, total, lambda p: p, mom_send, mom_recv)
    for copy in halo_copies:
        copy.wait_send()
    sums.wait_send()
    for side in range(2):
        pos = i + side * (n_layer - 1 - 2 * i)

        @pl.when(pos < n_layer - 1)
        def _():
            for part in range(2):
                relay_copy(side, part, gout.at[side]).wait_send()

    sums.wait_recv()
    gram = jnp.sum(mom[...].reshape(total, nz), axis=0, keepdims=True)

    def entry(a, b):
        k = names[min(a, b), max(a, b)]
        return gram[:, k : k + 1]

    def inner(x, y):
        terms = [x[a] * y[b] * entry(a, b) for a in x for b in y]
        return functools.reduce(lambda p, q: p + q, terms)

    def add(x, y, scale):
        out = dict(x)
        for k, val in y.items():
            out[k] = out[k] + scale * val if k in out else scale * val
        return out

    def apply(x):
        out = {}
        for k, val in x.items():
            out = add(out, {k: val}, CENTER)
            if k == 0:
                out = add(out, {1: val}, HALF)
            else:
                out = add(out, {k + 1: val, k - 1: val}, 0.5 * HALF)
        return out

    one = jnp.ones((1, 1), F32)
    pot, res, direction = {}, {0: one}, {0: one}
    norm = inner(res, res)
    for it in range(CG_ITERS):
        applied = apply(direction)
        step = norm / inner(direction, applied)
        pot = add(pot, direction, step)
        res = add(res, applied, -step)
        if it + 1 < CG_ITERS:
            new = inner(res, res)
            direction = add(res, direction, new / norm)
            norm = new

    for coefs, out in ((pot, pot_ref), (res, res_ref)):
        terms = [coefs[k][None] * own_v[k] for k in coefs]
        out[...] = functools.reduce(lambda p, q: p + q, terms)


def put(dens_ref, pot_ref, res_ref, dens_hbm, pot_hbm, res_hbm, sem):
    copies = [
        pltpu.make_async_copy(src, dst, sem.at[k])
        for k, (src, dst) in enumerate(((pot_ref, pot_hbm), (res_ref, res_hbm), (dens_ref, dens_hbm)))
    ]
    for copy in copies:
        copy.start()
    for copy in copies:
        copy.wait()


def body(n_energy, n_layer, layer_inverse, coupling, lead_left, lead_right, quad_weight,
         energy_slot, plane_of, doping, screening):
    steps, m = layer_inverse.shape[1], layer_inverse.shape[2]
    planes, ny, nz = doping.shape
    ext = planes + 2 * CG_ITERS
    dma = pltpu.SemaphoreType.DMA
    vmem = pl.BlockSpec(memory_space=pltpu.VMEM)
    anym = pl.BlockSpec(memory_space=pltpu.HBM)
    call = pl.pallas_call(
        functools.partial(kernel, n_energy, n_layer),
        out_shape=(pltpu.VMEM((steps, m), F32), pltpu.VMEM(doping.shape, F32), pltpu.VMEM(doping.shape, F32)),
        in_specs=[anym] * 9,
        out_specs=(vmem, vmem, vmem),
        scratch_shapes=[
            pltpu.VMEM((steps, m, m), F32),
            pltpu.VMEM((m, m), F32),
            pltpu.VMEM((1,) + quad_weight.shape, F32),
            pltpu.VMEM((1, 1), jnp.int32),
            pltpu.VMEM((1,) + plane_of.shape, jnp.int32),
            pltpu.VMEM(doping.shape, F32),
            pltpu.VMEM(doping.shape, F32),
            dma((steps + 8,)),
            pltpu.VMEM((2, 2, 2, m, m), BF16),
            pltpu.VMEM((2, m, m), F32),
            pltpu.VMEM((2, steps, 2, m, m), BF16),
            pltpu.VMEM((2, 2, m, m), BF16),
            pltpu.VMEM((2, steps, m, m), F32),
            pltpu.VMEM((2, m, m), BF16),
            pltpu.VMEM((2, steps, m), F32),
            pltpu.VMEM((steps, m), F32),
            pltpu.VMEM((2, m, m), F32),
            pltpu.VMEM((2, m, m), F32),
            pltpu.VMEM((ext, ny, nz), F32),
            pltpu.VMEM((ext, ny, nz), F32),
            pltpu.VMEM((n_energy, steps, m), F32),
            pltpu.VMEM((2 * n_layer, steps, m), F32),
            pltpu.VMEM((n_energy * n_layer, 1, nz), F32),
            dma((2, 2)), dma((2, 2)), dma((4,)), dma((4,)),
            dma, dma, dma, dma, dma, dma,
        ],
        compiler_params=pltpu.CompilerParams(
            collective_id=0, has_side_effects=True, vmem_limit_bytes=66_000_000
        ),
    )
    inner = call(
        layer_inverse[0], coupling, lead_left[0], lead_right[0], quad_weight[None, :],
        energy_slot[:, None], plane_of[None, :], doping, screening,
    )
    return pl.pallas_call(
        put,
        out_shape=tuple(jax.ShapeDtypeStruct(x.shape, F32) for x in inner),
        in_specs=[vmem] * 3,
        out_specs=(anym, anym, anym),
        scratch_shapes=[dma((3,))],
        compiler_params=pltpu.CompilerParams(vmem_limit_bytes=1_000_000),
    )(*(pltpu.with_memory_space_constraint(x, pltpu.VMEM) for x in inner))


def solution(mesh):
    in_specs = (
        P("energy", "layer", None, None),
        P(),
        P("energy", None, None),
        P("energy", None, None),
        P(),
        P("energy"),
        P(),
        P(("energy", "layer"), None, None),
        P(("energy", "layer"), None, None),
    )
    out_specs = (
        P("layer", None),
        P(("energy", "layer"), None, None),
        P(("energy", "layer"), None, None),
    )
    run = functools.partial(body, mesh.shape["energy"], mesh.shape["layer"])
    return jax.shard_map(run, mesh=mesh, in_specs=in_specs, out_specs=out_specs, check_vma=False)
```

```python
import functools
import jax
import jax.numpy as jnp
from jax import lax
from jax.experimental import pallas as pl
from jax.experimental.pallas import tpu as pltpu
from jax.sharding import PartitionSpec as P

ORB_Y = 16
CG_ITERS = 3
CENTER = 7.125
HALF = 7.0
F32 = jnp.float32
BF16 = jnp.bfloat16
LOGICAL = pl.DeviceIdType.LOGICAL


def split(x):
    hi = x.astype(BF16)
    lo = (x - hi.astype(F32)).astype(BF16)
    return hi, lo


def mm(a, b):
    return jnp.dot(a, b, preferred_element_type=F32)


def mm3(a, b, dot=mm):
    return dot(a[0], b[0]) + dot(a[0], b[1]) + dot(a[1], b[0])


def mmt(a, b):
    return lax.dot_general(a, b, (((1,), (1,)), ((), ())), preferred_element_type=F32)


def loop(count, step):
    if count <= 32:
        for k in range(1, count):
            step(k, 0)
    else:
        lax.fori_loop(1, count, step, 0)


def around(x):
    ny, nz = x.shape
    row = lax.broadcasted_iota(jnp.int32, (8, nz), 0)
    lane = lax.broadcasted_iota(jnp.int32, (1, nz), 1)
    up, down = pltpu.roll(x, 1, 0), pltpu.roll(x, ny - 1, 0)
    up = jnp.concatenate([jnp.where(row == 0, 0.0, up[:8]), up[8:]], axis=0)
    down = jnp.concatenate([down[:-8], jnp.where(row == 7, 0.0, down[-8:])], axis=0)
    left, right = pltpu.roll(x, 1, 1), pltpu.roll(x, nz - 1, 1)
    sides = jnp.where(lane == 0, right, jnp.where(lane == nz - 1, left, left + right))
    return (up + down) + sides


def kernel(
    n_energy, n_layer,
    d_hbm, t_hbm, lead_l_hbm, lead_r_hbm, qw_hbm, slot_hbm, plane_hbm, dop_hbm, scr_hbm,
    dens_ref, pot_ref, res_ref,
    d_ref, t_ref, qw_ref, slot_ref, plane_ref, dop_ref, scr_ref, in_sem,
    p_ref, s_ref, ct_ref, c_ref, w_ref, x_ref, diag_ref, full_ref, gin, gout, dop_ext, scr_ext,
    v_ref, coef_ref, spread_ref, zbuf, redbuf, mom,
    relay_send, relay_recv, halo_send, halo_recv,
    z_send, z_recv, red_send, red_recv, mom_send, mom_recv,
):
    steps, m, _ = d_hbm.shape
    planes, ny, nz = dop_hbm.shape
    halo = CG_ITERS
    ext = planes + 2 * halo
    total = n_energy * n_layer
    e = lax.axis_index("energy")
    i = lax.axis_index("layer")
    lin = e * n_layer + i
    up = lax.rem(lin + 1, total)
    down = lax.rem(lin + total - 1, total)

    order = []
    for s in range((steps + 1) // 2):
        order += [s] if s == steps - 1 - s else [s, steps - 1 - s]
    t_copy = pltpu.make_async_copy(t_hbm, t_ref, in_sem.at[steps + 4])
    t_copy.start()

    def layer_copy(s):
        return pltpu.make_async_copy(d_hbm.at[s], d_ref.at[s], in_sem.at[s])

    def lead_copy(side):
        return pltpu.make_async_copy((lead_l_hbm, lead_r_hbm)[side], s_ref.at[side], in_sem.at[steps + 2 + side])

    ends = (0, n_layer - 1)
    for s in order[:2]:
        layer_copy(s).start()
    for side in range(2):
        pl.when(i == ends[side])(lead_copy(side).start)
    for s in order[2:]:
        layer_copy(s).start()
    grid_copies = [
        pltpu.make_async_copy(qw_hbm, qw_ref, in_sem.at[steps + 5]),
        pltpu.make_async_copy(plane_hbm, plane_ref, in_sem.at[steps + 6]),
        pltpu.make_async_copy(slot_hbm, slot_ref, in_sem.at[steps + 7]),
        pltpu.make_async_copy(dop_hbm, dop_ref, in_sem.at[steps]),
        pltpu.make_async_copy(scr_hbm, scr_ref, in_sem.at[steps + 1]),
    ]
    for copy in grid_copies:
        copy.start()

    barrier = pltpu.get_barrier_semaphore()

    def greet(k, c):
        pl.semaphore_signal(barrier, inc=1, device_id=lax.rem(lin + k, total), device_id_type=LOGICAL)
        return c

    loop(total, greet)

    halo_copies = []
    for j, (src, dst, width) in enumerate(((dop_ref, dop_ext, halo), (scr_ref, scr_ext, halo - 1))):
        halo_copies.append(pltpu.make_async_remote_copy(
            src_ref=src.at[pl.ds(planes - width, width)], dst_ref=dst.at[pl.ds(halo - width, width)],
            send_sem=halo_send.at[2 * j], recv_sem=halo_recv.at[2 * j],
            device_id=up, device_id_type=LOGICAL))
        halo_copies.append(pltpu.make_async_remote_copy(
            src_ref=src.at[pl.ds(0, width)], dst_ref=dst.at[pl.ds(planes + halo, width)],
            send_sem=halo_send.at[2 * j + 1], recv_sem=halo_recv.at[2 * j + 1],
            device_id=down, device_id_type=LOGICAL))

    t_copy.wait()
    t = t_ref[...]
    tt = t.T
    t, tt = split(t), split(tt)
    eye = (lax.broadcasted_iota(jnp.int32, (m // 2, m // 2), 0)
           == lax.broadcasted_iota(jnp.int32, (m // 2, m // 2), 1))

    def diag_row(x):
        h = m // 2
        tiles = [jnp.where(eye, x[k * h : k * h + h, k * h : k * h + h], 0.0) for k in range(2)]
        return jnp.concatenate([jnp.sum(tile, axis=0, keepdims=True) for tile in tiles], axis=1)

    sides = ((t, tt), (tt, t))
    h = m // 2
    last = steps - 1

    def layer_of(side, s):
        return s if side == 0 else last - s

    def pair(ref, at):
        return ref[at + (0,)], ref[at + (1,)]

    def prepare(s, side):
        prop = mm3(split(d_ref[layer_of(side, s)]), sides[side][0])
        for j, x in enumerate(split(prop)):
            p_ref[side, s % 2, j] = x

    def store_carry(s, side, ct):
        hi, lo = split(ct)
        ct_ref[side, s, 0] = hi
        ct_ref[side, s, 1] = lo
        w_ref[side, s] = 2.0 * ct - hi.astype(F32)

    for side in range(2):
        @pl.when(i != ends[side])
        def _():
            s_ref[side] = jnp.zeros((m, m), F32)
    for s in order[:2]:
        layer_copy(s).wait()
    for side in range(2):
        prepare(0, side)
    for s in order[2:]:
        layer_copy(s).wait()
    for side in range(2):
        pl.when(i == ends[side])(lead_copy(side).wait)

    for s in range(steps):
        props = [pair(p_ref, (side, s % 2)) for side in range(2)]
        halves = []
        for side in range(2):
            s_hi, s_lo = split(s_ref[side])
            halves.append(mm(props[side][0], s_hi) + mm(props[side][0], s_lo))
        if s < last:
            for side in range(2):
                prepare(s + 1, side)
        for side in range(2):
            d = d_ref[layer_of(side, s)]
            hi, lo = split(halves[side])
            cross = mmt(hi, props[side][1])
            acc = d + (mmt(hi, props[side][0]) + mmt(lo, props[side][0])) + (cross + cross.T)
            s_ref[side] = acc
            diag_ref[side, s : s + 1, :] = diag_row(acc)
            if side == 0:
                full_ref[s : s + 1, :] = diag_row(d)
        for side in range(2):
            if s == 0:
                hi, lo = (x.T for x in props[side])
                ct_ref[side, 0, 0] = hi
                ct_ref[side, 0, 1] = lo
                w_ref[side, 0] = hi.astype(F32) + 2.0 * lo.astype(F32)
            else:
                store_carry(s, side, mm3(pair(ct_ref, (side, s - 1)), props[side], mmt))
        if s == 1:
            pl.semaphore_wait(barrier, total - 1)
            for copy in grid_copies:
                copy.wait()
            for copy in halo_copies:
                copy.start()

    def relay_copy(side, part, buf):
        spot = (pl.ds(0, h), pl.ds(0, m)) if part == 0 else (pl.ds(h, h), pl.ds(h, h))
        return pltpu.make_async_remote_copy(
            src_ref=buf.at[spot], dst_ref=gin.at[(side,) + spot],
            send_sem=relay_send.at[side, part], recv_sem=relay_recv.at[side, part],
            device_id=e * n_layer + lax.rem(i + 1 - 2 * side + n_layer, n_layer), device_id_type=LOGICAL)

    for side in range(2):
        @pl.when(i == ends[side])
        def _():
            for part in range(2):
                relay_copy(side, part, s_ref.at[side]).start()

    for side in range(2):
        for part in range(2):
            c_ref[side, part] = ct_ref[side, last, part].T

    first = (2 * i) // n_layer

    first_plane = lin * planes - halo

    def inside(q):
        return jnp.logical_and(first_plane + q >= 0, first_plane + q < total * planes)

    def turn_step(turn, c):
        side = first + turn * (1 - 2 * first)
        pos = i + side * (n_layer - 1 - 2 * i)

        @pl.when(turn == 1)
        def _():
            for copy in halo_copies:
                copy.wait_recv()
            for q in range(ext):
                keep = inside(q)
                own = halo <= q < halo + planes
                dop = dop_ref[q - halo] if own else dop_ext[q]
                dop_ext[q] = jnp.where(keep, dop, 0.0)
                if 0 < q < ext - 1:
                    scr = scr_ref[q - halo] if own else scr_ext[q]
                    coef_ref[q] = jnp.where(keep, (6.0 - CENTER + scr) * (1.0 / HALF), 0.0)

        @pl.when(pos > 0)
        def _():
            relay_copy(side, 0, gout.at[side]).wait_recv()
            gin[side, h:, :h] = gin[side, :h, h:].T
            relay_copy(side, 1, gout.at[side]).wait_recv()
            for part, x in enumerate(split(gin[side])):
                x_ref[part] = x

            @pl.when(pos < n_layer - 1)
            def _():
                half = split(mm3((x_ref[0], x_ref[1]), pair(ct_ref, (side, last))))
                outer = pair(c_ref, (side,))
                gout[side, :h, :] = s_ref[side, :h, :] + mm3([x[:h] for x in outer], half)
                relay_copy(side, 0, gout.at[side]).start()
                gout[side, h:, h:] = (
                    s_ref[side, h:, h:] + mm3([x[h:] for x in outer], [x[:, h:] for x in half]))
                relay_copy(side, 1, gout.at[side]).start()

            for s in range(steps):
                carry = ct_ref[side, s, 0]
                z = mm(x_ref[0], carry) + mm(x_ref[1], carry)
                diag_ref[side, s : s + 1, :] += jnp.sum(z * w_ref[side, s], axis=0, keepdims=True)

        return c

    lax.fori_loop(0, 2, turn_step, 0)

    n_slots = qw_ref.shape[1]
    pick = lax.broadcasted_iota(jnp.int32, (1, n_slots), 1) == slot_ref[...]
    weight = jnp.sum(jnp.where(pick, qw_ref[...], 0.0), axis=1, keepdims=True)
    back = jnp.concatenate([diag_ref[1, steps - 1 - s : steps - s, :] for s in range(steps)], axis=0)
    near = 2 if n_energy % 2 == 0 else 1
    far = n_energy // near
    zed = e // near
    ring = near * n_layer
    own = lax.rem(lin, ring)
    zbuf[zed] = weight * (diag_ref[0] + back - full_ref[...])

    def exchange(buf, me, count, place, send_sem, recv_sem):
        def send(k, c):
            pltpu.make_async_remote_copy(
                src_ref=buf.at[me], dst_ref=buf.at[me], send_sem=send_sem, recv_sem=recv_sem,
                device_id=place(lax.rem(me + k, count)), device_id_type=LOGICAL).start()
            return c

        loop(count, send)
        rest = buf.at[pl.ds(0, count - 1)]
        return pltpu.make_async_remote_copy(
            src_ref=rest, dst_ref=rest, send_sem=send_sem, recv_sem=recv_sem,
            device_id=place(lax.rem(me + 1, count)), device_id_type=LOGICAL)

    def ordered_sum(ref, count, start=0, stride=1):
        if count <= 8:
            out = ref[start]
            for k in range(1, count):
                out = out + ref[start + k * stride]
            return out
        return lax.fori_loop(1, count, lambda k, c: c + ref[start + k * stride], ref[start])

    wide = exchange(zbuf, zed, far, lambda p: p * ring + own, z_send, z_recv)
    wide.wait_recv()
    redbuf[own] = ordered_sum(zbuf, far)
    red = exchange(redbuf, own, ring, lambda p: zed * ring + p, red_send, red_recv)
    wide.wait_send()
    red.wait_recv()
    red.wait_send()
    rows = [ordered_sum(redbuf, near, k, n_layer) for k in range(n_layer)]
    dens_ref[...] = ordered_sum(redbuf, near, i, n_layer)

    rows = split(jnp.concatenate(rows, axis=0))
    orb_z = m // ORB_Y
    padded = -(-ext // 8) * 8
    ids = first_plane + lax.broadcasted_iota(jnp.int32, (padded, 1), 0)
    onehot = (plane_ref[...] == ids).astype(F32).astype(BF16)
    charge_rows = mm(onehot, rows[0]) + mm(onehot, rows[1])
    ysel = (lax.broadcasted_iota(jnp.int32, (ORB_Y, m), 1) // orb_z
            == lax.broadcasted_iota(jnp.int32, (ORB_Y, m), 0))
    zsel = (lax.broadcasted_iota(jnp.int32, (m, nz), 1) // (nz // orb_z)
            == lax.rem(lax.broadcasted_iota(jnp.int32, (m, nz), 0), orb_z)).astype(BF16)
    spreads = split(jnp.concatenate(
        [jnp.where(ysel, charge_rows[p : p + 1, :], 0.0) for p in range(ext)], axis=0))
    spread_ref[...] = mm(spreads[0], zsel) + mm(spreads[1], zsel)
    patch = ny // ORB_Y
    for q in range(ext):
        charge = [jnp.broadcast_to(spread_ref[q * ORB_Y + y : q * ORB_Y + y + 1, :], (patch, nz)) for y in range(ORB_Y)]
        v_ref[0, q] = jnp.concatenate(charge, axis=0) - dop_ext[q]
    for k in range(1, CG_ITERS + 1):
        twice = 1.0 if k == 1 else 2.0
        for q in range(k, ext - k):
            scale = jnp.where(inside(q), twice / HALF, 0.0)
            x = v_ref[k - 1, q]
            near_sum = (v_ref[k - 1, q - 1] + v_ref[k - 1, q + 1]) + around(x)
            out = twice * coef_ref[q] * x - scale * near_sum
            v_ref[k, q] = out if k == 1 else out - v_ref[k - 2, q]

    def dot_of(a, b):
        out = 0.0
        for q in range(halo, halo + planes):
            prod = v_ref[a, q] * v_ref[b, q]
            out = out + jnp.sum(prod.reshape(ny // 8, 8, nz), axis=0)
        return jnp.sum(out, axis=0, keepdims=True)

    pairs = [(0, k) for k in range(CG_ITERS + 1)] + [(CG_ITERS - 1, k) for k in range(CG_ITERS - 1, CG_ITERS + 1)]
    parts = [dot_of(a, b) for a, b in pairs]
    parts.append(jnp.zeros((8 - len(parts), nz), F32))
    column = jnp.sum(jnp.concatenate(parts, axis=0), axis=1, keepdims=True)
    spot = lax.broadcasted_iota(jnp.int32, (8, nz), 0) == lax.broadcasted_iota(jnp.int32, (8, nz), 1)
    mom[lin] = jnp.sum(jnp.where(spot, column, 0.0), axis=0, keepdims=True)

    sums = exchange(mom, lin, total, lambda p: p, mom_send, mom_recv)
    for copy in halo_copies:
        copy.wait_send()
    sums.wait_send()
    for side in range(2):
        pos = i + side * (n_layer - 1 - 2 * i)

        @pl.when(pos < n_layer - 1)
        def _():
            for part in range(2):
                relay_copy(side, part, gout.at[side]).wait_send()

    sums.wait_recv()
    gram = jnp.sum(mom[...].reshape(total, nz), axis=0, keepdims=True)

    base = [gram[:, k : k + 1] for k in range(len(pairs))]
    moments = base[: CG_ITERS + 1]
    moments += [2.0 * base[CG_ITERS + 1 + k] - moments[k] for k in range(2)]

    def entry(a, b):
        return 0.5 * (moments[a + b] + moments[abs(a - b)])

    def inner(x, y):
        terms = [x[a] * y[b] * entry(a, b) for a in x for b in y]
        return functools.reduce(lambda p, q: p + q, terms)

    def add(x, y, scale):
        out = dict(x)
        for k, val in y.items():
            out[k] = out[k] + scale * val if k in out else scale * val
        return out

    def apply(x):
        out = {}
        for k, val in x.items():
            out = add(out, {k: val}, CENTER)
            if k == 0:
                out = add(out, {1: val}, HALF)
            else:
                out = add(out, {k + 1: val, k - 1: val}, 0.5 * HALF)
        return out

    one = jnp.ones((1, 1), F32)
    pot, res, direction = {}, {0: one}, {0: one}
    norm = inner(res, res)
    for it in range(CG_ITERS):
        applied = apply(direction)
        step = norm / inner(direction, applied)
        pot = add(pot, direction, step)
        res = add(res, applied, -step)
        if it + 1 < CG_ITERS:
            new = inner(res, res)
            direction = add(res, direction, new / norm)
            norm = new

    for coefs, out in ((pot, pot_ref), (res, res_ref)):
        for q in range(planes):
            terms = [coefs[k] * v_ref[k, halo + q] for k in coefs]
            out[q] = functools.reduce(lambda p, q: p + q, terms)


def put(dens_ref, pot_ref, res_ref, dens_hbm, pot_hbm, res_hbm, sem):
    copies = [
        pltpu.make_async_copy(src, dst, sem.at[k])
        for k, (src, dst) in enumerate(((pot_ref, pot_hbm), (res_ref, res_hbm), (dens_ref, dens_hbm)))
    ]
    for copy in copies:
        copy.start()
    for copy in copies:
        copy.wait()


def body(n_energy, n_layer, layer_inverse, coupling, lead_left, lead_right, quad_weight,
         energy_slot, plane_of, doping, screening):
    steps, m = layer_inverse.shape[1], layer_inverse.shape[2]
    planes, ny, nz = doping.shape
    ext = planes + 2 * CG_ITERS
    dma = pltpu.SemaphoreType.DMA
    vmem = pl.BlockSpec(memory_space=pltpu.VMEM)
    anym = pl.BlockSpec(memory_space=pltpu.HBM)
    call = pl.pallas_call(
        functools.partial(kernel, n_energy, n_layer),
        out_shape=(pltpu.VMEM((steps, m), F32), pltpu.VMEM(doping.shape, F32), pltpu.VMEM(doping.shape, F32)),
        in_specs=[anym] * 9,
        out_specs=(vmem, vmem, vmem),
        scratch_shapes=[
            pltpu.VMEM((steps, m, m), F32),
            pltpu.VMEM((m, m), F32),
            pltpu.VMEM((1,) + quad_weight.shape, F32),
            pltpu.VMEM((1, 1), jnp.int32),
            pltpu.VMEM((1,) + plane_of.shape, jnp.int32),
            pltpu.VMEM(doping.shape, F32),
            pltpu.VMEM(doping.shape, F32),
            dma((steps + 8,)),
            pltpu.VMEM((2, 2, 2, m, m), BF16),
            pltpu.VMEM((2, m, m), F32),
            pltpu.VMEM((2, steps, 2, m, m), BF16),
            pltpu.VMEM((2, 2, m, m), BF16),
            pltpu.VMEM((2, steps, m, m), F32),
            pltpu.VMEM((2, m, m), BF16),
            pltpu.VMEM((2, steps, m), F32),
            pltpu.VMEM((steps, m), F32),
            pltpu.VMEM((2, m, m), F32),
            pltpu.VMEM((2, m, m), F32),
            pltpu.VMEM((ext, ny, nz), F32),
            pltpu.VMEM((ext, ny, nz), F32),
            pltpu.VMEM((CG_ITERS + 1, ext, ny, nz), F32),
            pltpu.VMEM((ext, ny, nz), F32),
            pltpu.VMEM((ext * ORB_Y, nz), F32),
            pltpu.VMEM((n_energy, steps, m), F32),
            pltpu.VMEM((2 * n_layer, steps, m), F32),
            pltpu.VMEM((n_energy * n_layer, 1, nz), F32),
            dma((2, 2)), dma((2, 2)), dma((4,)), dma((4,)),
            dma, dma, dma, dma, dma, dma,
        ],
        compiler_params=pltpu.CompilerParams(
            collective_id=0, has_side_effects=True, vmem_limit_bytes=66_000_000
        ),
    )
    inner = call(
        layer_inverse[0], coupling, lead_left[0], lead_right[0], quad_weight[None, :],
        energy_slot[:, None], plane_of[None, :], doping, screening,
    )
    return pl.pallas_call(
        put,
        out_shape=tuple(jax.ShapeDtypeStruct(x.shape, F32) for x in inner),
        in_specs=[vmem] * 3,
        out_specs=(anym, anym, anym),
        scratch_shapes=[dma((3,))],
        compiler_params=pltpu.CompilerParams(vmem_limit_bytes=1_000_000),
    )(*(pltpu.with_memory_space_constraint(x, pltpu.VMEM) for x in inner))


def solution(mesh):
    in_specs = (
        P("energy", "layer", None, None),
        P(),
        P("energy", None, None),
        P("energy", None, None),
        P(),
        P("energy"),
        P(),
        P(("energy", "layer"), None, None),
        P(("energy", "layer"), None, None),
    )
    out_specs = (
        P("layer", None),
        P(("energy", "layer"), None, None),
        P(("energy", "layer"), None, None),
    )
    run = functools.partial(body, mesh.shape["energy"], mesh.shape["layer"])
    return jax.shard_map(run, mesh=mesh, in_specs=in_specs, out_specs=out_specs, check_vma=False)
```

```python
import functools
import jax
import jax.numpy as jnp
from jax import lax
from jax.experimental import pallas as pl
from jax.experimental.pallas import tpu as pltpu
from jax.sharding import PartitionSpec as P

ORB_Y = 16
CG_ITERS = 3
CENTER = 7.125
HALF = 7.0
F32 = jnp.float32
BF16 = jnp.bfloat16
LOGICAL = pl.DeviceIdType.LOGICAL


def split(x):
    hi = x.astype(BF16)
    lo = (x - hi.astype(F32)).astype(BF16)
    return hi, lo


def mm(a, b):
    return jnp.dot(a, b, preferred_element_type=F32)


def mm3(a, b, dot=mm):
    return dot(a[0], b[0]) + dot(a[0], b[1]) + dot(a[1], b[0])


def mmt(a, b):
    return lax.dot_general(a, b, (((1,), (1,)), ((), ())), preferred_element_type=F32)


def loop(count, step):
    if count <= 32:
        for k in range(1, count):
            step(k, 0)
    else:
        lax.fori_loop(1, count, step, 0)


def around(x):
    ny, nz = x.shape
    row = lax.broadcasted_iota(jnp.int32, (8, nz), 0)
    lane = lax.broadcasted_iota(jnp.int32, (1, nz), 1)
    up, down = pltpu.roll(x, 1, 0), pltpu.roll(x, ny - 1, 0)
    up = jnp.concatenate([jnp.where(row == 0, 0.0, up[:8]), up[8:]], axis=0)
    down = jnp.concatenate([down[:-8], jnp.where(row == 7, 0.0, down[-8:])], axis=0)
    left, right = pltpu.roll(x, 1, 1), pltpu.roll(x, nz - 1, 1)
    sides = jnp.where(lane == 0, right, jnp.where(lane == nz - 1, left, left + right))
    return (up + down) + sides


def kernel(
    n_energy, n_layer,
    d_hbm, t_hbm, lead_l_hbm, lead_r_hbm, qw_hbm, slot_hbm, plane_hbm, dop_hbm, scr_hbm,
    dens_ref, pot_ref, res_ref,
    d_ref, t_ref, qw_ref, slot_ref, plane_ref, dop_ref, scr_ref, in_sem,
    p_ref, s_ref, ct_ref, c_ref, w_ref, x_ref, diag_ref, full_ref, gin, gout, dop_ext, scr_ext,
    v_ref, coef_ref, spread_ref, zbuf, redbuf, mom, pair_ref,
    pair_send, pair_recv, relay_send, relay_recv, halo_send, halo_recv,
    z_send, z_recv, red_send, red_recv, mom_send, mom_recv,
):
    steps, m, _ = d_hbm.shape
    planes, ny, nz = dop_hbm.shape
    halo = CG_ITERS
    ext = planes + 2 * halo
    total = n_energy * n_layer
    e = lax.axis_index("energy")
    i = lax.axis_index("layer")
    lin = e * n_layer + i
    up = lax.rem(lin + 1, total)
    down = lax.rem(lin + total - 1, total)

    order = []
    for s in range((steps + 1) // 2):
        order += [s] if s == steps - 1 - s else [s, steps - 1 - s]
    t_copy = pltpu.make_async_copy(t_hbm, t_ref, in_sem.at[steps + 4])
    t_copy.start()

    def layer_copy(s):
        return pltpu.make_async_copy(d_hbm.at[s], d_ref.at[s], in_sem.at[s])

    def lead_copy(side):
        return pltpu.make_async_copy((lead_l_hbm, lead_r_hbm)[side], s_ref.at[side], in_sem.at[steps + 2 + side])

    ends = (0, n_layer - 1)
    for s in order[:2]:
        layer_copy(s).start()
    for side in range(2):
        pl.when(i == ends[side])(lead_copy(side).start)
    for s in order[2:]:
        layer_copy(s).start()
    grid_copies = [
        pltpu.make_async_copy(qw_hbm, qw_ref, in_sem.at[steps + 5]),
        pltpu.make_async_copy(plane_hbm, plane_ref, in_sem.at[steps + 6]),
        pltpu.make_async_copy(slot_hbm, slot_ref, in_sem.at[steps + 7]),
        pltpu.make_async_copy(dop_hbm, dop_ref, in_sem.at[steps]),
        pltpu.make_async_copy(scr_hbm, scr_ref, in_sem.at[steps + 1]),
    ]
    for copy in grid_copies:
        copy.start()

    barrier = pltpu.get_barrier_semaphore()

    def greet(k, c):
        pl.semaphore_signal(barrier, inc=1, device_id=lax.rem(lin + k, total), device_id_type=LOGICAL)
        return c

    loop(total, greet)

    halo_copies = []
    for j, (src, dst, width) in enumerate(((dop_ref, dop_ext, halo), (scr_ref, scr_ext, halo - 1))):
        halo_copies.append(pltpu.make_async_remote_copy(
            src_ref=src.at[pl.ds(planes - width, width)], dst_ref=dst.at[pl.ds(halo - width, width)],
            send_sem=halo_send.at[2 * j], recv_sem=halo_recv.at[2 * j],
            device_id=up, device_id_type=LOGICAL))
        halo_copies.append(pltpu.make_async_remote_copy(
            src_ref=src.at[pl.ds(0, width)], dst_ref=dst.at[pl.ds(planes + halo, width)],
            send_sem=halo_send.at[2 * j + 1], recv_sem=halo_recv.at[2 * j + 1],
            device_id=down, device_id_type=LOGICAL))

    t_copy.wait()
    t = t_ref[...]
    tt = t.T
    t, tt = split(t), split(tt)
    eye = (lax.broadcasted_iota(jnp.int32, (m // 2, m // 2), 0)
           == lax.broadcasted_iota(jnp.int32, (m // 2, m // 2), 1))

    def diag_row(x):
        h = m // 2
        tiles = [jnp.where(eye, x[k * h : k * h + h, k * h : k * h + h], 0.0) for k in range(2)]
        return jnp.concatenate([jnp.sum(tile, axis=0, keepdims=True) for tile in tiles], axis=1)

    sides = ((t, tt), (tt, t))
    h = m // 2
    last = steps - 1

    def layer_of(side, s):
        return s if side == 0 else last - s

    def pair(ref, at):
        return ref[at + (0,)], ref[at + (1,)]

    def prepare(s, side):
        prop = mm3(split(d_ref[layer_of(side, s)]), sides[side][0])
        for j, x in enumerate(split(prop)):
            p_ref[side, s % 2, j] = x

    def store_carry(s, side, ct):
        hi, lo = split(ct)
        ct_ref[side, s, 0] = hi
        ct_ref[side, s, 1] = lo
        w_ref[side, s] = 2.0 * ct - hi.astype(F32)

    for side in range(2):
        @pl.when(i != ends[side])
        def _():
            s_ref[side] = jnp.zeros((m, m), F32)
    for s in order[:2]:
        layer_copy(s).wait()
    for side in range(2):
        prepare(0, side)
    for s in order[2:]:
        layer_copy(s).wait()
    for side in range(2):
        pl.when(i == ends[side])(lead_copy(side).wait)

    pairs = n_layer == 4
    for s in range(steps):
        props = [pair(p_ref, (side, s % 2)) for side in range(2)]
        halves = []
        for side in range(2):
            s_hi, s_lo = split(s_ref[side])
            halves.append(mm(props[side][0], s_hi) + mm(props[side][0], s_lo))
        if s < last:
            for side in range(2):
                prepare(s + 1, side)
        for side in range(2):
            d = d_ref[layer_of(side, s)]
            hi, lo = split(halves[side])
            cross = mmt(hi, props[side][1])
            acc = d + (mmt(hi, props[side][0]) + mmt(lo, props[side][0])) + (cross + cross.T)
            s_ref[side] = acc
            diag_ref[side, s : s + 1, :] = diag_row(acc)
            if side == 0:
                full_ref[s : s + 1, :] = diag_row(d)
        for side in range(2):
            if s == 0:
                hi, lo = (x.T for x in props[side])
                ct_ref[side, 0, 0] = hi
                ct_ref[side, 0, 1] = lo
                w_ref[side, 0] = hi.astype(F32) + 2.0 * lo.astype(F32)
            else:
                ct = mm3(pair(ct_ref, (side, s - 1)), props[side], mmt)
                store_carry(s, side, ct)
                if pairs and s == last:
                    gout[side] = ct
        if s == 1:
            pl.semaphore_wait(barrier, total - 1)
            for copy in grid_copies:
                copy.wait()
            for copy in halo_copies:
                copy.start()

    def relay_copy(side, part, buf):
        spot = (pl.ds(0, h), pl.ds(0, m)) if part == 0 else (pl.ds(h, h), pl.ds(h, h))
        return pltpu.make_async_remote_copy(
            src_ref=buf.at[spot], dst_ref=gin.at[(side,) + spot],
            send_sem=relay_send.at[side, part], recv_sem=relay_recv.at[side, part],
            device_id=e * n_layer + lax.rem(i + 1 - 2 * side + n_layer, n_layer), device_id_type=LOGICAL)

    for side in range(2):
        @pl.when(i == ends[side])
        def _():
            for part in range(2):
                relay_copy(side, part, s_ref.at[side]).start()

    def pair_copy(side, part):
        return pltpu.make_async_remote_copy(
            src_ref=(s_ref, gout)[part].at[side], dst_ref=pair_ref.at[part],
            send_sem=pair_send.at[part], recv_sem=pair_recv.at[part],
            device_id=e * n_layer + lax.rem(i + 1 - 2 * side + n_layer, n_layer), device_id_type=LOGICAL)

    if pairs:
        for side in range(2):
            @pl.when(i == 2 - side)
            def _():
                for part in range(2):
                    pair_copy(side, part).start()

    for side in range(2):
        for part in range(2):
            c_ref[side, part] = ct_ref[side, last, part].T

    first = (2 * i) // n_layer

    first_plane = lin * planes - halo

    def inside(q):
        return jnp.logical_and(first_plane + q >= 0, first_plane + q < total * planes)

    def turn_step(turn, c):
        side = first + turn * (1 - 2 * first)
        pos = i + side * (n_layer - 1 - 2 * i)

        @pl.when(turn == 1)
        def _():
            for copy in halo_copies:
                copy.wait_recv()
            for q in range(ext):
                keep = inside(q)
                own = halo <= q < halo + planes
                dop = dop_ref[q - halo] if own else dop_ext[q]
                dop_ext[q] = jnp.where(keep, dop, 0.0)
                if 0 < q < ext - 1:
                    scr = scr_ref[q - halo] if own else scr_ext[q]
                    coef_ref[q] = jnp.where(keep, (6.0 - CENTER + scr) * (1.0 / HALF), 0.0)

        if pairs:
            @pl.when(pos == 3)
            def _():
                for part in range(2):
                    pair_copy(side, part).wait_recv()
                below = split(pair_ref[0])
                outer = split(pair_ref[1])
                for s in range(steps):
                    cur = pair(ct_ref, (side, s))
                    z = mm(below[0], cur[0]) + mm(below[1], cur[0])
                    diag_ref[side, s : s + 1, :] += jnp.sum(z * w_ref[side, s], axis=0, keepdims=True)
                    store_carry(s, side, mm3(outer, cur))

        relays = pos == 1 if pairs else jnp.logical_and(pos > 0, pos < n_layer - 1)
        ends_here = pos > 1 if pairs else pos == n_layer - 1

        def take(part):
            relay_copy(side, part, gout.at[side]).wait_recv()

        def fill(part):
            rows = slice(0, h) if part == 0 else slice(h, m)
            if part == 1:
                gin[side, h:, :h] = gin[side, :h, h:].T
            for k, x in enumerate(split(gin[side, rows, :])):
                x_ref[k, rows, :] = x

        def forward(part):
            if pairs:
                @pl.when(pos == 2)
                def _():
                    relay_copy(side, part, gin.at[side]).start()

        def apply(part):
            rows = slice(0, h) if part == 0 else slice(h, m)
            for s in range(steps):
                carry = ct_ref[side, s, 0]
                z = mm(x_ref[0, rows, :], carry) + mm(x_ref[1, rows, :], carry)
                diag_ref[side, s : s + 1, :] += jnp.sum(z * w_ref[side, s, rows, :], axis=0, keepdims=True)

        @pl.when(relays)
        def _():
            for part in range(2):
                take(part)
                fill(part)
            half = split(mm3((x_ref[0], x_ref[1]), pair(ct_ref, (side, last))))
            outer = pair(c_ref, (side,))
            gout[side, :h, :] = s_ref[side, :h, :] + mm3([x[:h] for x in outer], half)
            relay_copy(side, 0, gout.at[side]).start()
            gout[side, h:, h:] = (
                s_ref[side, h:, h:] + mm3([x[h:] for x in outer], [x[:, h:] for x in half]))
            relay_copy(side, 1, gout.at[side]).start()

        for part in range(2):
            @pl.when(ends_here)
            def _():
                take(part)
                forward(part)
                fill(part)

            pl.when(pos > 0)(functools.partial(apply, part))

        return c

    lax.fori_loop(0, 2, turn_step, 0)

    n_slots = qw_ref.shape[1]
    pick = lax.broadcasted_iota(jnp.int32, (1, n_slots), 1) == slot_ref[...]
    weight = jnp.sum(jnp.where(pick, qw_ref[...], 0.0), axis=1, keepdims=True)
    back = jnp.concatenate([diag_ref[1, steps - 1 - s : steps - s, :] for s in range(steps)], axis=0)
    near = 2 if n_energy % 2 == 0 else 1
    far = n_energy // near
    zed = e // near
    ring = near * n_layer
    own = lax.rem(lin, ring)
    zbuf[zed] = weight * (diag_ref[0] + back - full_ref[...])

    def exchange(buf, me, count, place, send_sem, recv_sem):
        def send(k, c):
            pltpu.make_async_remote_copy(
                src_ref=buf.at[me], dst_ref=buf.at[me], send_sem=send_sem, recv_sem=recv_sem,
                device_id=place(lax.rem(me + k, count)), device_id_type=LOGICAL).start()
            return c

        loop(count, send)
        rest = buf.at[pl.ds(0, count - 1)]
        return pltpu.make_async_remote_copy(
            src_ref=rest, dst_ref=rest, send_sem=send_sem, recv_sem=recv_sem,
            device_id=place(lax.rem(me + 1, count)), device_id_type=LOGICAL)

    def ordered_sum(ref, count, start=0, stride=1):
        if count <= 8:
            out = ref[start]
            for k in range(1, count):
                out = out + ref[start + k * stride]
            return out
        return lax.fori_loop(1, count, lambda k, c: c + ref[start + k * stride], ref[start])

    wide = exchange(zbuf, zed, far, lambda p: p * ring + own, z_send, z_recv)
    wide.wait_recv()
    redbuf[own] = ordered_sum(zbuf, far)
    red = exchange(redbuf, own, ring, lambda p: zed * ring + p, red_send, red_recv)
    wide.wait_send()
    red.wait_recv()
    red.wait_send()
    rows = [ordered_sum(redbuf, near, k, n_layer) for k in range(n_layer)]
    dens_ref[...] = ordered_sum(redbuf, near, i, n_layer)

    rows = split(jnp.concatenate(rows, axis=0))
    orb_z = m // ORB_Y
    padded = -(-ext // 8) * 8
    ids = first_plane + lax.broadcasted_iota(jnp.int32, (padded, 1), 0)
    onehot = (plane_ref[...] == ids).astype(F32).astype(BF16)
    charge_rows = mm(onehot, rows[0]) + mm(onehot, rows[1])
    ysel = (lax.broadcasted_iota(jnp.int32, (ORB_Y, m), 1) // orb_z
            == lax.broadcasted_iota(jnp.int32, (ORB_Y, m), 0))
    zsel = (lax.broadcasted_iota(jnp.int32, (m, nz), 1) // (nz // orb_z)
            == lax.rem(lax.broadcasted_iota(jnp.int32, (m, nz), 0), orb_z)).astype(BF16)
    spreads = split(jnp.concatenate(
        [jnp.where(ysel, charge_rows[p : p + 1, :], 0.0) for p in range(ext)], axis=0))
    spread_ref[...] = mm(spreads[0], zsel) + mm(spreads[1], zsel)
    patch = ny // ORB_Y
    for q in range(ext):
        charge = [jnp.broadcast_to(spread_ref[q * ORB_Y + y : q * ORB_Y + y + 1, :], (patch, nz)) for y in range(ORB_Y)]
        v_ref[0, q] = jnp.concatenate(charge, axis=0) - dop_ext[q]
    for k in range(1, CG_ITERS + 1):
        twice = 1.0 if k == 1 else 2.0
        for q in range(k, ext - k):
            scale = jnp.where(inside(q), twice / HALF, 0.0)
            x = v_ref[k - 1, q]
            near_sum = (v_ref[k - 1, q - 1] + v_ref[k - 1, q + 1]) + around(x)
            out = twice * coef_ref[q] * x - scale * near_sum
            v_ref[k, q] = out if k == 1 else out - v_ref[k - 2, q]

    def dot_of(a, b):
        out = 0.0
        for q in range(halo, halo + planes):
            prod = v_ref[a, q] * v_ref[b, q]
            out = out + jnp.sum(prod.reshape(ny // 8, 8, nz), axis=0)
        return jnp.sum(out, axis=0, keepdims=True)

    pairs = [(0, k) for k in range(CG_ITERS + 1)] + [(CG_ITERS - 1, k) for k in range(CG_ITERS - 1, CG_ITERS + 1)]
    parts = [dot_of(a, b) for a, b in pairs]
    parts.append(jnp.zeros((8 - len(parts), nz), F32))
    column = jnp.sum(jnp.concatenate(parts, axis=0), axis=1, keepdims=True)
    spot = lax.broadcasted_iota(jnp.int32, (8, nz), 0) == lax.broadcasted_iota(jnp.int32, (8, nz), 1)
    mom[lin] = jnp.sum(jnp.where(spot, column, 0.0), axis=0, keepdims=True)

    sums = exchange(mom, lin, total, lambda p: p, mom_send, mom_recv)
    for copy in halo_copies:
        copy.wait_send()
    sums.wait_send()
    for side in range(2):
        pos = i + side * (n_layer - 1 - 2 * i)

        @pl.when(pos < n_layer - 1)
        def _():
            for part in range(2):
                relay_copy(side, part, gout.at[side]).wait_send()

    if pairs:
        for side in range(2):
            @pl.when(i == 2 - side)
            def _():
                for part in range(2):
                    pair_copy(side, part).wait_send()

    sums.wait_recv()
    gram = jnp.sum(mom[...].reshape(total, nz), axis=0, keepdims=True)

    base = [gram[:, k : k + 1] for k in range(len(pairs))]
    moments = base[: CG_ITERS + 1]
    moments += [2.0 * base[CG_ITERS + 1 + k] - moments[k] for k in range(2)]

    def entry(a, b):
        return 0.5 * (moments[a + b] + moments[abs(a - b)])

    def inner(x, y):
        terms = [x[a] * y[b] * entry(a, b) for a in x for b in y]
        return functools.reduce(lambda p, q: p + q, terms)

    def add(x, y, scale):
        out = dict(x)
        for k, val in y.items():
            out[k] = out[k] + scale * val if k in out else scale * val
        return out

    def apply(x):
        out = {}
        for k, val in x.items():
            out = add(out, {k: val}, CENTER)
            if k == 0:
                out = add(out, {1: val}, HALF)
            else:
                out = add(out, {k + 1: val, k - 1: val}, 0.5 * HALF)
        return out

    one = jnp.ones((1, 1), F32)
    pot, res, direction = {}, {0: one}, {0: one}
    norm = inner(res, res)
    for it in range(CG_ITERS):
        applied = apply(direction)
        step = norm / inner(direction, applied)
        pot = add(pot, direction, step)
        res = add(res, applied, -step)
        if it + 1 < CG_ITERS:
            new = inner(res, res)
            direction = add(res, direction, new / norm)
            norm = new

    for coefs, out in ((pot, pot_ref), (res, res_ref)):
        for q in range(planes):
            terms = [coefs[k] * v_ref[k, halo + q] for k in coefs]
            out[q] = functools.reduce(lambda p, q: p + q, terms)


def put(dens_ref, pot_ref, res_ref, dens_hbm, pot_hbm, res_hbm, sem):
    copies = [
        pltpu.make_async_copy(src, dst, sem.at[k])
        for k, (src, dst) in enumerate(((pot_ref, pot_hbm), (res_ref, res_hbm), (dens_ref, dens_hbm)))
    ]
    for copy in copies:
        copy.start()
    for copy in copies:
        copy.wait()


def body(n_energy, n_layer, layer_inverse, coupling, lead_left, lead_right, quad_weight,
         energy_slot, plane_of, doping, screening):
    steps, m = layer_inverse.shape[1], layer_inverse.shape[2]
    planes, ny, nz = doping.shape
    ext = planes + 2 * CG_ITERS
    dma = pltpu.SemaphoreType.DMA
    vmem = pl.BlockSpec(memory_space=pltpu.VMEM)
    anym = pl.BlockSpec(memory_space=pltpu.HBM)
    call = pl.pallas_call(
        functools.partial(kernel, n_energy, n_layer),
        out_shape=(pltpu.VMEM((steps, m), F32), pltpu.VMEM(doping.shape, F32), pltpu.VMEM(doping.shape, F32)),
        in_specs=[anym] * 9,
        out_specs=(vmem, vmem, vmem),
        scratch_shapes=[
            pltpu.VMEM((steps, m, m), F32),
            pltpu.VMEM((m, m), F32),
            pltpu.VMEM((1,) + quad_weight.shape, F32),
            pltpu.VMEM((1, 1), jnp.int32),
            pltpu.VMEM((1,) + plane_of.shape, jnp.int32),
            pltpu.VMEM(doping.shape, F32),
            pltpu.VMEM(doping.shape, F32),
            dma((steps + 8,)),
            pltpu.VMEM((2, 2, 2, m, m), BF16),
            pltpu.VMEM((2, m, m), F32),
            pltpu.VMEM((2, steps, 2, m, m), BF16),
            pltpu.VMEM((2, 2, m, m), BF16),
            pltpu.VMEM((2, steps, m, m), F32),
            pltpu.VMEM((2, m, m), BF16),
            pltpu.VMEM((2, steps, m), F32),
            pltpu.VMEM((steps, m), F32),
            pltpu.VMEM((2, m, m), F32),
            pltpu.VMEM((2, m, m), F32),
            pltpu.VMEM((ext, ny, nz), F32),
            pltpu.VMEM((ext, ny, nz), F32),
            pltpu.VMEM((CG_ITERS + 1, ext, ny, nz), F32),
            pltpu.VMEM((ext, ny, nz), F32),
            pltpu.VMEM((ext * ORB_Y, nz), F32),
            pltpu.VMEM((n_energy, steps, m), F32),
            pltpu.VMEM((2 * n_layer, steps, m), F32),
            pltpu.VMEM((n_energy * n_layer, 1, nz), F32),
            pltpu.VMEM((2, m, m), F32),
            dma((2,)), dma((2,)),
            dma((2, 2)), dma((2, 2)), dma((4,)), dma((4,)),
            dma, dma, dma, dma, dma, dma,
        ],
        compiler_params=pltpu.CompilerParams(
            collective_id=0, has_side_effects=True, vmem_limit_bytes=66_000_000
        ),
    )
    inner = call(
        layer_inverse[0], coupling, lead_left[0], lead_right[0], quad_weight[None, :],
        energy_slot[:, None], plane_of[None, :], doping, screening,
    )
    return pl.pallas_call(
        put,
        out_shape=tuple(jax.ShapeDtypeStruct(x.shape, F32) for x in inner),
        in_specs=[vmem] * 3,
        out_specs=(anym, anym, anym),
        scratch_shapes=[dma((3,))],
        compiler_params=pltpu.CompilerParams(vmem_limit_bytes=1_000_000),
    )(*(pltpu.with_memory_space_constraint(x, pltpu.VMEM) for x in inner))


def solution(mesh):
    in_specs = (
        P("energy", "layer", None, None),
        P(),
        P("energy", None, None),
        P("energy", None, None),
        P(),
        P("energy"),
        P(),
        P(("energy", "layer"), None, None),
        P(("energy", "layer"), None, None),
    )
    out_specs = (
        P("layer", None),
        P(("energy", "layer"), None, None),
        P(("energy", "layer"), None, None),
    )
    run = functools.partial(body, mesh.shape["energy"], mesh.shape["layer"])
    return jax.shard_map(run, mesh=mesh, in_specs=in_specs, out_specs=out_specs, check_vma=False)
```

```python
import functools
import jax
import jax.numpy as jnp
from jax import lax
from jax.experimental import pallas as pl
from jax.experimental.pallas import tpu as pltpu
from jax.sharding import PartitionSpec as P

ORB_Y = 16
CG_ITERS = 3
CENTER = 7.125
HALF = 7.0
F32 = jnp.float32
BF16 = jnp.bfloat16
LOGICAL = pl.DeviceIdType.LOGICAL


def split(x):
    hi = x.astype(BF16)
    lo = (x - hi.astype(F32)).astype(BF16)
    return hi, lo


def mm(a, b):
    return jnp.dot(a, b, preferred_element_type=F32)


def mm3(a, b, dot=mm):
    return dot(a[0], b[0]) + dot(a[0], b[1]) + dot(a[1], b[0])


def mmt(a, b):
    return lax.dot_general(a, b, (((1,), (1,)), ((), ())), preferred_element_type=F32)


def loop(count, step):
    if count <= 32:
        for k in range(1, count):
            step(k, 0)
    else:
        lax.fori_loop(1, count, step, 0)


def around(x):
    ny, nz = x.shape
    row = lax.broadcasted_iota(jnp.int32, (8, nz), 0)
    lane = lax.broadcasted_iota(jnp.int32, (1, nz), 1)
    up, down = pltpu.roll(x, 1, 0), pltpu.roll(x, ny - 1, 0)
    up = jnp.concatenate([jnp.where(row == 0, 0.0, up[:8]), up[8:]], axis=0)
    down = jnp.concatenate([down[:-8], jnp.where(row == 7, 0.0, down[-8:])], axis=0)
    left, right = pltpu.roll(x, 1, 1), pltpu.roll(x, nz - 1, 1)
    sides = jnp.where(lane == 0, right, jnp.where(lane == nz - 1, left, left + right))
    return (up + down) + sides


def kernel(
    n_energy, n_layer,
    d_hbm, t_hbm, lead_l_hbm, lead_r_hbm, qw_hbm, slot_hbm, plane_hbm, dop_hbm, scr_hbm,
    dens_ref, pot_ref, res_ref,
    d_ref, t_ref, qw_ref, slot_ref, plane_ref, dop_ref, scr_ref, in_sem,
    p_ref, s_ref, ct_ref, c_ref, w_ref, x_ref, diag_ref, full_ref, gin, gout, dop_ext, scr_ext,
    v_ref, coef_ref, spread_ref, zbuf, redbuf, mom, pair_ref,
    pair_send, pair_recv, relay_send, relay_recv, halo_send, halo_recv,
    z_send, z_recv, red_send, red_recv, mom_send, mom_recv,
):
    steps, m, _ = d_hbm.shape
    planes, ny, nz = dop_hbm.shape
    halo = CG_ITERS
    ext = planes + 2 * halo
    total = n_energy * n_layer
    e = lax.axis_index("energy")
    i = lax.axis_index("layer")
    lin = e * n_layer + i
    up = lax.rem(lin + 1, total)
    down = lax.rem(lin + total - 1, total)

    order = []
    for s in range((steps + 1) // 2):
        order += [s] if s == steps - 1 - s else [s, steps - 1 - s]
    t_copy = pltpu.make_async_copy(t_hbm, t_ref, in_sem.at[steps + 4])
    t_copy.start()

    def layer_copy(s):
        return pltpu.make_async_copy(d_hbm.at[s], d_ref.at[s], in_sem.at[s])

    def lead_copy(side):
        return pltpu.make_async_copy((lead_l_hbm, lead_r_hbm)[side], s_ref.at[side], in_sem.at[steps + 2 + side])

    ends = (0, n_layer - 1)
    at_end = jnp.logical_or(i == 0, i == n_layer - 1)
    for s in order[:2]:
        layer_copy(s).start()
    for side in range(2):
        pl.when(i == ends[side])(lead_copy(side).start)
    for s in order[2:]:
        layer_copy(s).start()
    grid_copies = [
        pltpu.make_async_copy(qw_hbm, qw_ref, in_sem.at[steps + 5]),
        pltpu.make_async_copy(plane_hbm, plane_ref, in_sem.at[steps + 6]),
        pltpu.make_async_copy(slot_hbm, slot_ref, in_sem.at[steps + 7]),
        pltpu.make_async_copy(dop_hbm, dop_ref, in_sem.at[steps]),
        pltpu.make_async_copy(scr_hbm, scr_ref, in_sem.at[steps + 1]),
    ]
    for copy in grid_copies:
        copy.start()

    barrier = pltpu.get_barrier_semaphore()

    def greet(k, c):
        pl.semaphore_signal(barrier, inc=1, device_id=lax.rem(lin + k, total), device_id_type=LOGICAL)
        return c

    loop(total, greet)

    halo_copies = []
    for j, (src, dst, width) in enumerate(((dop_ref, dop_ext, halo), (scr_ref, scr_ext, halo - 1))):
        halo_copies.append(pltpu.make_async_remote_copy(
            src_ref=src.at[pl.ds(planes - width, width)], dst_ref=dst.at[pl.ds(halo - width, width)],
            send_sem=halo_send.at[2 * j], recv_sem=halo_recv.at[2 * j],
            device_id=up, device_id_type=LOGICAL))
        halo_copies.append(pltpu.make_async_remote_copy(
            src_ref=src.at[pl.ds(0, width)], dst_ref=dst.at[pl.ds(planes + halo, width)],
            send_sem=halo_send.at[2 * j + 1], recv_sem=halo_recv.at[2 * j + 1],
            device_id=down, device_id_type=LOGICAL))

    t_copy.wait()
    t = split(t_ref[...])
    eye = (lax.broadcasted_iota(jnp.int32, (m // 2, m // 2), 0)
           == lax.broadcasted_iota(jnp.int32, (m // 2, m // 2), 1))

    def diag_row(x):
        h = m // 2
        tiles = [jnp.where(eye, x[k * h : k * h + h, k * h : k * h + h], 0.0) for k in range(2)]
        return jnp.concatenate([jnp.sum(tile, axis=0, keepdims=True) for tile in tiles], axis=1)

    dots = (mm, mmt)
    h = m // 2
    last = steps - 1

    def layer_of(side, s):
        return s if side == 0 else last - s

    def pair(ref, at):
        return ref[at + (0,)], ref[at + (1,)]

    def prepare(s, side):
        prop = mm3(split(d_ref[layer_of(side, s)]), t, dots[side])
        for j, x in enumerate(split(prop)):
            p_ref[side, s % 2, j] = x

    def store_carry(s, side, ct):
        hi, lo = split(ct)
        ct_ref[side, s, 0] = hi
        ct_ref[side, s, 1] = lo
        w_ref[side, s] = 2.0 * ct - hi.astype(F32)

    for side in range(2):
        @pl.when(i != ends[side])
        def _():
            s_ref[side] = jnp.zeros((m, m), F32)
    for s in order[:2]:
        layer_copy(s).wait()
    for side in range(2):
        prepare(0, side)
    for s in order[2:]:
        layer_copy(s).wait()
    for side in range(2):
        pl.when(i == ends[side])(lead_copy(side).wait)

    def relay_copy(side, part, buf):
        spot = (pl.ds(0, h), pl.ds(0, m)) if part == 0 else (pl.ds(h, h), pl.ds(h, h))
        return pltpu.make_async_remote_copy(
            src_ref=buf.at[spot], dst_ref=gin.at[(side,) + spot],
            send_sem=relay_send.at[side, part], recv_sem=relay_recv.at[side, part],
            device_id=e * n_layer + lax.rem(i + 1 - 2 * side + n_layer, n_layer), device_id_type=LOGICAL)

    pairs = n_layer == 4
    for s in range(steps):
        props = [pair(p_ref, (side, s % 2)) for side in range(2)]
        halves = []
        for side in range(2):
            s_hi, s_lo = split(s_ref[side])
            halves.append(mm(props[side][0], s_hi) + mm(props[side][0], s_lo))
        if s < last:
            for side in range(2):
                prepare(s + 1, side)
        for side in range(2):
            d = d_ref[layer_of(side, s)]
            hi, lo = split(halves[side])
            cross = mmt(hi, props[side][1])
            acc = d + (mmt(hi, props[side][0]) + mmt(lo, props[side][0])) + (cross + cross.T)
            s_ref[side] = acc
            diag_ref[side, s : s + 1, :] = diag_row(acc)
            if side == 0:
                full_ref[s : s + 1, :] = diag_row(d)
        if s == last:
            for side in range(2):
                @pl.when(i == ends[side])
                def _():
                    for part in range(2):
                        relay_copy(side, part, s_ref.at[side]).start()
        for side in range(2):
            if s == 0:
                hi, lo = (x.T for x in props[side])
                ct_ref[side, 0, 0] = hi
                ct_ref[side, 0, 1] = lo
                w_ref[side, 0] = hi.astype(F32) + 2.0 * lo.astype(F32)
            else:
                store_carry(s, side, mm3(pair(ct_ref, (side, s - 1)), props[side], mmt))
        if s == 1:
            pl.semaphore_wait(barrier, total - 1)
            for copy in grid_copies:
                copy.wait()
            for copy in halo_copies[:2]:
                copy.start()

            @pl.when(at_end)
            def _():
                for copy in halo_copies[2:]:
                    copy.start()

    def pair_copy(side, part):
        return pltpu.make_async_remote_copy(
            src_ref=(s_ref, gout)[part].at[side], dst_ref=pair_ref.at[part],
            send_sem=pair_send.at[part], recv_sem=pair_recv.at[part],
            device_id=e * n_layer + lax.rem(i + 1 - 2 * side + n_layer, n_layer), device_id_type=LOGICAL)

    if pairs:
        for side in range(2):
            @pl.when(i == 2 - side)
            def _():
                hi, lo = pair(ct_ref, (side, last))
                gout[side] = hi.astype(F32) + lo.astype(F32)
                for part in range(2):
                    pair_copy(side, part).start()

    for side in range(2):
        for part in range(2):
            c_ref[side, part] = ct_ref[side, last, part].T

    first = (2 * i) // n_layer

    first_plane = lin * planes - halo

    def inside(q):
        return jnp.logical_and(first_plane + q >= 0, first_plane + q < total * planes)

    def turn_step(turn, c):
        side = first + turn * (1 - 2 * first)
        pos = i + side * (n_layer - 1 - 2 * i)

        @pl.when(jnp.logical_and(turn == 1, jnp.logical_not(at_end)))
        def _():
            for copy in halo_copies[2:]:
                copy.start()

        if pairs:
            @pl.when(pos == 3)
            def _():
                for part in range(2):
                    pair_copy(side, part).wait_recv()
                below = split(pair_ref[0])
                outer = split(pair_ref[1])
                for s in range(steps):
                    cur = pair(ct_ref, (side, s))
                    z = mm(below[0], cur[0]) + mm(below[1], cur[0])
                    diag_ref[side, s : s + 1, :] += jnp.sum(z * w_ref[side, s], axis=0, keepdims=True)
                    store_carry(s, side, mm3(outer, cur))

        relays = pos == 1 if pairs else jnp.logical_and(pos > 0, pos < n_layer - 1)
        ends_here = pos > 1 if pairs else pos == n_layer - 1

        def take(part):
            relay_copy(side, part, gout.at[side]).wait_recv()

        def fill(part):
            rows = slice(0, h) if part == 0 else slice(h, m)
            if part == 1:
                gin[side, h:, :h] = gin[side, :h, h:].T
            for k, x in enumerate(split(gin[side, rows, :])):
                x_ref[k, rows, :] = x

        def forward(part):
            if pairs:
                @pl.when(pos == 2)
                def _():
                    relay_copy(side, part, gin.at[side]).start()

        def apply(part):
            rows = slice(0, h) if part == 0 else slice(h, m)
            for s in range(steps):
                carry = ct_ref[side, s, 0]
                z = mm(x_ref[0, rows, :], carry) + mm(x_ref[1, rows, :], carry)
                diag_ref[side, s : s + 1, :] += jnp.sum(z * w_ref[side, s, rows, :], axis=0, keepdims=True)

        @pl.when(relays)
        def _():
            for part in range(2):
                take(part)
                fill(part)
            half = split(mm3((x_ref[0], x_ref[1]), pair(ct_ref, (side, last))))
            outer = pair(c_ref, (side,))
            gout[side, :h, :] = s_ref[side, :h, :] + mm3([x[:h] for x in outer], half)
            relay_copy(side, 0, gout.at[side]).start()
            gout[side, h:, h:] = (
                s_ref[side, h:, h:] + mm3([x[h:] for x in outer], [x[:, h:] for x in half]))
            relay_copy(side, 1, gout.at[side]).start()

        for part in range(2):
            @pl.when(ends_here)
            def _():
                take(part)
                forward(part)
                fill(part)

            pl.when(pos > 0)(functools.partial(apply, part))

        return c

    lax.fori_loop(0, 2, turn_step, 0)

    n_slots = qw_ref.shape[1]
    pick = lax.broadcasted_iota(jnp.int32, (1, n_slots), 1) == slot_ref[...]
    weight = jnp.sum(jnp.where(pick, qw_ref[...], 0.0), axis=1, keepdims=True)
    back = jnp.concatenate([diag_ref[1, steps - 1 - s : steps - s, :] for s in range(steps)], axis=0)
    near = 2 if n_energy % 2 == 0 else 1
    far = n_energy // near
    zed = e // near
    ring = near * n_layer
    own = lax.rem(lin, ring)
    zbuf[zed] = weight * (diag_ref[0] + back - full_ref[...])

    def exchange(buf, me, count, place, send_sem, recv_sem):
        def send(k, c):
            pltpu.make_async_remote_copy(
                src_ref=buf.at[me], dst_ref=buf.at[me], send_sem=send_sem, recv_sem=recv_sem,
                device_id=place(lax.rem(me + k, count)), device_id_type=LOGICAL).start()
            return c

        loop(count, send)
        rest = buf.at[pl.ds(0, count - 1)]
        return pltpu.make_async_remote_copy(
            src_ref=rest, dst_ref=rest, send_sem=send_sem, recv_sem=recv_sem,
            device_id=place(lax.rem(me + 1, count)), device_id_type=LOGICAL)

    def ordered_sum(ref, count, start=0, stride=1):
        if count <= 8:
            out = ref[start]
            for k in range(1, count):
                out = out + ref[start + k * stride]
            return out
        return lax.fori_loop(1, count, lambda k, c: c + ref[start + k * stride], ref[start])

    wide = exchange(zbuf, zed, far, lambda p: p * ring + own, z_send, z_recv)
    for copy in halo_copies:
        copy.wait_recv()
    for q in range(ext):
        keep = inside(q)
        mine = halo <= q < halo + planes
        dop = dop_ref[q - halo] if mine else dop_ext[q]
        dop_ext[q] = jnp.where(keep, dop, 0.0)
        if 0 < q < ext - 1:
            scr = scr_ref[q - halo] if mine else scr_ext[q]
            coef_ref[q] = jnp.where(keep, (6.0 - CENTER + scr) * (1.0 / HALF), 0.0)
    wide.wait_recv()
    redbuf[own] = ordered_sum(zbuf, far)
    red = exchange(redbuf, own, ring, lambda p: zed * ring + p, red_send, red_recv)
    wide.wait_send()
    red.wait_recv()
    red.wait_send()
    rows = [ordered_sum(redbuf, near, k, n_layer) for k in range(n_layer)]
    dens_ref[...] = ordered_sum(redbuf, near, i, n_layer)

    rows = split(jnp.concatenate(rows, axis=0))
    orb_z = m // ORB_Y
    padded = -(-ext // 8) * 8
    ids = first_plane + lax.broadcasted_iota(jnp.int32, (padded, 1), 0)
    onehot = (plane_ref[...] == ids).astype(F32).astype(BF16)
    charge_rows = mm(onehot, rows[0]) + mm(onehot, rows[1])
    ysel = (lax.broadcasted_iota(jnp.int32, (ORB_Y, m), 1) // orb_z
            == lax.broadcasted_iota(jnp.int32, (ORB_Y, m), 0))
    zsel = (lax.broadcasted_iota(jnp.int32, (m, nz), 1) // (nz // orb_z)
            == lax.rem(lax.broadcasted_iota(jnp.int32, (m, nz), 0), orb_z)).astype(BF16)
    spreads = split(jnp.concatenate(
        [jnp.where(ysel, charge_rows[p : p + 1, :], 0.0) for p in range(ext)], axis=0))
    spread_ref[...] = mm(spreads[0], zsel) + mm(spreads[1], zsel)
    patch = ny // ORB_Y
    for q in range(ext):
        charge = [jnp.broadcast_to(spread_ref[q * ORB_Y + y : q * ORB_Y + y + 1, :], (patch, nz)) for y in range(ORB_Y)]
        v_ref[0, q] = jnp.concatenate(charge, axis=0) - dop_ext[q]
    for k in range(1, CG_ITERS + 1):
        twice = 1.0 if k == 1 else 2.0
        for q in range(k, ext - k):
            scale = jnp.where(inside(q), twice / HALF, 0.0)
            x = v_ref[k - 1, q]
            near_sum = (v_ref[k - 1, q - 1] + v_ref[k - 1, q + 1]) + around(x)
            out = twice * coef_ref[q] * x - scale * near_sum
            v_ref[k, q] = out if k == 1 else out - v_ref[k - 2, q]

    def dot_of(a, b):
        out = 0.0
        for q in range(halo, halo + planes):
            prod = v_ref[a, q] * v_ref[b, q]
            out = out + jnp.sum(prod.reshape(ny // 8, 8, nz), axis=0)
        return jnp.sum(out, axis=0, keepdims=True)

    pairs = [(0, k) for k in range(CG_ITERS + 1)] + [(CG_ITERS - 1, k) for k in range(CG_ITERS - 1, CG_ITERS + 1)]
    parts = [dot_of(a, b) for a, b in pairs]
    parts.append(jnp.zeros((8 - len(parts), nz), F32))
    column = jnp.sum(jnp.concatenate(parts, axis=0), axis=1, keepdims=True)
    spot = lax.broadcasted_iota(jnp.int32, (8, nz), 0) == lax.broadcasted_iota(jnp.int32, (8, nz), 1)
    mom[lin] = jnp.sum(jnp.where(spot, column, 0.0), axis=0, keepdims=True)

    sums = exchange(mom, lin, total, lambda p: p, mom_send, mom_recv)
    for copy in halo_copies:
        copy.wait_send()
    sums.wait_send()
    for side in range(2):
        pos = i + side * (n_layer - 1 - 2 * i)

        @pl.when(pos < n_layer - 1)
        def _():
            for part in range(2):
                relay_copy(side, part, gout.at[side]).wait_send()

    if pairs:
        for side in range(2):
            @pl.when(i == 2 - side)
            def _():
                for part in range(2):
                    pair_copy(side, part).wait_send()

    sums.wait_recv()
    gram = jnp.sum(mom[...].reshape(total, nz), axis=0, keepdims=True)

    base = [gram[:, k : k + 1] for k in range(len(pairs))]
    moments = base[: CG_ITERS + 1]
    moments += [2.0 * base[CG_ITERS + 1 + k] - moments[k] for k in range(2)]

    def entry(a, b):
        return 0.5 * (moments[a + b] + moments[abs(a - b)])

    def inner(x, y):
        terms = [x[a] * y[b] * entry(a, b) for a in x for b in y]
        return functools.reduce(lambda p, q: p + q, terms)

    def add(x, y, scale):
        out = dict(x)
        for k, val in y.items():
            out[k] = out[k] + scale * val if k in out else scale * val
        return out

    def apply(x):
        out = {}
        for k, val in x.items():
            out = add(out, {k: val}, CENTER)
            if k == 0:
                out = add(out, {1: val}, HALF)
            else:
                out = add(out, {k + 1: val, k - 1: val}, 0.5 * HALF)
        return out

    one = jnp.ones((1, 1), F32)
    pot, res, direction = {}, {0: one}, {0: one}
    norm = inner(res, res)
    for it in range(CG_ITERS):
        applied = apply(direction)
        step = norm / inner(direction, applied)
        pot = add(pot, direction, step)
        res = add(res, applied, -step)
        if it + 1 < CG_ITERS:
            new = inner(res, res)
            direction = add(res, direction, new / norm)
            norm = new

    for coefs, out in ((pot, pot_ref), (res, res_ref)):
        for q in range(planes):
            terms = [coefs[k] * v_ref[k, halo + q] for k in coefs]
            out[q] = functools.reduce(lambda p, q: p + q, terms)


def put(dens_ref, pot_ref, res_ref, dens_hbm, pot_hbm, res_hbm, sem):
    copies = [
        pltpu.make_async_copy(src, dst, sem.at[k])
        for k, (src, dst) in enumerate(((pot_ref, pot_hbm), (res_ref, res_hbm), (dens_ref, dens_hbm)))
    ]
    for copy in copies:
        copy.start()
    for copy in copies:
        copy.wait()


def body(n_energy, n_layer, layer_inverse, coupling, lead_left, lead_right, quad_weight,
         energy_slot, plane_of, doping, screening):
    steps, m = layer_inverse.shape[1], layer_inverse.shape[2]
    planes, ny, nz = doping.shape
    ext = planes + 2 * CG_ITERS
    dma = pltpu.SemaphoreType.DMA
    vmem = pl.BlockSpec(memory_space=pltpu.VMEM)
    anym = pl.BlockSpec(memory_space=pltpu.HBM)
    call = pl.pallas_call(
        functools.partial(kernel, n_energy, n_layer),
        out_shape=(pltpu.VMEM((steps, m), F32), pltpu.VMEM(doping.shape, F32), pltpu.VMEM(doping.shape, F32)),
        in_specs=[anym] * 9,
        out_specs=(vmem, vmem, vmem),
        scratch_shapes=[
            pltpu.VMEM((steps, m, m), F32),
            pltpu.VMEM((m, m), F32),
            pltpu.VMEM((1,) + quad_weight.shape, F32),
            pltpu.VMEM((1, 1), jnp.int32),
            pltpu.VMEM((1,) + plane_of.shape, jnp.int32),
            pltpu.VMEM(doping.shape, F32),
            pltpu.VMEM(doping.shape, F32),
            dma((steps + 8,)),
            pltpu.VMEM((2, 2, 2, m, m), BF16),
            pltpu.VMEM((2, m, m), F32),
            pltpu.VMEM((2, steps, 2, m, m), BF16),
            pltpu.VMEM((2, 2, m, m), BF16),
            pltpu.VMEM((2, steps, m, m), F32),
            pltpu.VMEM((2, m, m), BF16),
            pltpu.VMEM((2, steps, m), F32),
            pltpu.VMEM((steps, m), F32),
            pltpu.VMEM((2, m, m), F32),
            pltpu.VMEM((2, m, m), F32),
            pltpu.VMEM((ext, ny, nz), F32),
            pltpu.VMEM((ext, ny, nz), F32),
            pltpu.VMEM((CG_ITERS + 1, ext, ny, nz), F32),
            pltpu.VMEM((ext, ny, nz), F32),
            pltpu.VMEM((ext * ORB_Y, nz), F32),
            pltpu.VMEM((n_energy, steps, m), F32),
            pltpu.VMEM((2 * n_layer, steps, m), F32),
            pltpu.VMEM((n_energy * n_layer, 1, nz), F32),
            pltpu.VMEM((2, m, m), F32),
            dma((2,)), dma((2,)),
            dma((2, 2)), dma((2, 2)), dma((4,)), dma((4,)),
            dma, dma, dma, dma, dma, dma,
        ],
        compiler_params=pltpu.CompilerParams(
            collective_id=0, has_side_effects=True, vmem_limit_bytes=66_000_000
        ),
    )
    inner = call(
        layer_inverse[0], coupling, lead_left[0], lead_right[0], quad_weight[None, :],
        energy_slot[:, None], plane_of[None, :], doping, screening,
    )
    return pl.pallas_call(
        put,
        out_shape=tuple(jax.ShapeDtypeStruct(x.shape, F32) for x in inner),
        in_specs=[vmem] * 3,
        out_specs=(anym, anym, anym),
        scratch_shapes=[dma((3,))],
        compiler_params=pltpu.CompilerParams(vmem_limit_bytes=1_000_000),
    )(*(pltpu.with_memory_space_constraint(x, pltpu.VMEM) for x in inner))


def solution(mesh):
    in_specs = (
        P("energy", "layer", None, None),
        P(),
        P("energy", None, None),
        P("energy", None, None),
        P(),
        P("energy"),
        P(),
        P(("energy", "layer"), None, None),
        P(("energy", "layer"), None, None),
    )
    out_specs = (
        P("layer", None),
        P(("energy", "layer"), None, None),
        P(("energy", "layer"), None, None),
    )
    run = functools.partial(body, mesh.shape["energy"], mesh.shape["layer"])
    return jax.shard_map(run, mesh=mesh, in_specs=in_specs, out_specs=out_specs, check_vma=False)
```
